256 devices in a mesh: gx: 2 (over y_lo), gy: 32 (over y_hi, z, core), gz: 4 (over x).
Axes of the slice: x: 4, y: 4 (y_hi: 2, y_lo: 2; y = y_hi * 2 + y_lo), z: 8, core: 2. Of those that a mesh axis runs over, the one named last changes fastest.
Arguments:
- velocity: float32 [3, 256, 256, 512], P(None, 'gy', 'gx', 'gz'), may hold values from -6 to 6
- stress: float32 [6, 256, 256, 512], P(None, 'gy', 'gx', 'gz'), may hold values from -6 to 6
- buoyancy: float32 [256, 256, 512], P('gy', 'gx', 'gz'), may hold values from 0.5 to 2
- stiff_xx: float32 [256, 256, 512], P('gy', 'gx', 'gz'), may hold values from 2 to 4
- stiff_xz: float32 [256, 256, 512], P('gy', 'gx', 'gz'), may hold values from 0.5 to 1
- stiff_zz: float32 [256, 256, 512], P('gy', 'gx', 'gz'), may hold values from 1.5 to 3
- shear_vert: float32 [256, 256, 512], P('gy', 'gx', 'gz'), may hold values from 0.5 to 1
- shear_horiz: float32 [256, 256, 512], P('gy', 'gx', 'gz'), may hold values from 0.6 to 1.2
- prestress: float32 [2, 256, 512], P(None, 'gy', 'gz'), may hold values from -24 to 24
- fault_mask: int32 [256, 512], P('gy', 'gz'), may hold values 0 or 1
- region_ids: int32 [256, 512], P('gy', 'gz'), may hold values from 0 to 7
- inverse_rate: float32 [256, 512], P('gy', 'gz'), may hold values from 100 to 10000
- slip_prev: float32 [256, 512], P('gy', 'gz'), may hold values from 0.01 to 2
- region_a: float32 [8], replicated, may hold values from 0.01 to 0.04
- region_normal: float32 [8], replicated, may hold values from 20 to 60
Outputs:
- new_velocity: float32 [3, 256, 256, 512], P(None, 'gy', 'gx', 'gz')
- new_stress: float32 [6, 256, 256, 512], P(None, 'gy', 'gx', 'gz')
- slip_rate: float32 [256, 512], P('gy', 'gz')
The draws below stay inside these ranges and needn't reach their ends.
All inputs are finite; a program needn't handle non-finite values. No bound on the sum of `fault_mask` on one device may be relied on, other than what follows from the above.
Results may differ from the reference program's by a relative error of at most 0.0003.
Values sent between devices are 32-bit elements; how exact they have to be, the bound alone decides.
A program may use at most 128 MiB of HBM per device.

```python
import math
import jax
import jax.numpy as jnp
from jax import lax

STEPS = 3
NEWTON = 3
REGIONS = 8
NY = 256
NX = 256
NZ = 512


def touch_ends(values, key, least, top_value):
    extent = values.shape
    spot = [jax.random.randint(jax.random.fold_in(key, axis), (), 0, extent[axis]) for axis in range(len(extent))]
    values = values.at[tuple(spot)].set(least)
    longest = extent.index(max(extent))
    spot[longest] = (spot[longest] + 1) % extent[longest]
    return values.at[tuple(spot)].set(top_value)


def steps_of(stream_key, dims, cuts, low, largest):
    loudness, own = 1.0, jax.random.fold_in(stream_key, 6)
    for axis_at, parts in cuts:
        heights = jnp.exp(jax.random.uniform(jax.random.fold_in(own, axis_at), (parts,), jnp.float32, low / len(cuts), largest / len(cuts)))
        loudness = loudness * jnp.repeat(heights, dims[axis_at] // parts).reshape([-1 if axis == axis_at else 1 for axis in range(len(dims))])
    return loudness


def noise(key, shape, deviation, reach, cuts=(), held_as=jnp.bfloat16):
    entries = deviation * jax.random.normal(key, shape, jnp.float32)
    if cuts:
        entries = entries * steps_of(key, shape, cuts, -0.22, 0.18)
    return jnp.clip(entries, -reach, reach).astype(held_as)


def setup_inputs(seed: int = 0) -> dict:
    splits = jax.random.split(jax.random.key(seed), 16)
    return {
        "velocity": noise(splits[0], (3, NY, NX, NZ), 1.0, 6.0, ((1, 32), (2, 2), (3, 4)), jnp.float32),
        "stress": noise(splits[1], (6, NY, NX, NZ), 1.0, 6.0, ((1, 32), (2, 2), (3, 4)), jnp.float32),
        "buoyancy": jnp.clip(jnp.exp(math.log(2.0) - 1.3862944 * jax.random.uniform(splits[2], (NY, NX, NZ), jnp.float32) ** steps_of(splits[2], (NY, NX, NZ), ((0, 32), (1, 2), (2, 4)), -0.2, 0.2)), 0.5, 2.0),
        "stiff_xx": jnp.clip(2.0 + 2.0 * jax.random.uniform(splits[3], (NY, NX, NZ), jnp.float32) ** steps_of(splits[3], (NY, NX, NZ), ((0, 32), (1, 2), (2, 4)), -0.2, 0.2), 2.0, 4.0),
        "stiff_xz": jnp.clip(0.5 + 0.5 * jax.random.uniform(splits[4], (NY, NX, NZ), jnp.float32) ** steps_of(splits[4], (NY, NX, NZ), ((0, 32), (1, 2), (2, 4)), -0.2, 0.2), 0.5, 1.0),
        "stiff_zz": jnp.clip(1.5 + 1.5 * jax.random.uniform(splits[5], (NY, NX, NZ), jnp.float32) ** steps_of(splits[5], (NY, NX, NZ), ((0, 32), (1, 2), (2, 4)), -0.2, 0.2), 1.5, 3.0),
        "shear_vert": jnp.clip(0.5 + 0.5 * jax.random.uniform(splits[6], (NY, NX, NZ), jnp.float32) ** steps_of(splits[6], (NY, NX, NZ), ((0, 32), (1, 2), (2, 4)), -0.2, 0.2), 0.5, 1.0),
        "shear_horiz": jnp.clip(0.6 + 0.6 * jax.random.uniform(splits[7], (NY, NX, NZ), jnp.float32) ** steps_of(splits[7], (NY, NX, NZ), ((0, 32), (1, 2), (2, 4)), -0.2, 0.2), 0.6, 1.2),
        "prestress": noise(splits[8], (2, NY, NZ), 6.0, 24.0, ((1, 32), (2, 4)), jnp.float32),
        "fault_mask": touch_ends((jax.random.randint(splits[9], (NY, NZ), 0, 4) < 3).astype(jnp.int32), jax.random.fold_in(splits[9], 1), 0, 1),
        "region_ids": touch_ends(jax.random.randint(splits[10], (NY, NZ), 0, REGIONS), jax.random.fold_in(splits[10], 1), 0, REGIONS - 1).astype(jnp.int32),
        "inverse_rate": jnp.clip(jnp.exp(math.log(10000.0) - 4.6051702 * jax.random.uniform(splits[11], (NY, NZ), jnp.float32) ** steps_of(splits[11], (NY, NZ), ((0, 32), (1, 4)), -0.2, 0.2)), 100.0, 10000.0),
        "slip_prev": jnp.clip(jnp.exp(math.log(2.0) - 5.2983174 * jax.random.uniform(splits[12], (NY, NZ), jnp.float32) ** steps_of(splits[12], (NY, NZ), ((0, 32), (1, 4)), -0.2, 0.2)), 0.01, 2.0),
        "region_a": jnp.clip(jnp.exp(jax.random.uniform(splits[13], (REGIONS,), jnp.float32, math.log(0.01), math.log(0.04))), 0.01, 0.04),
        "region_normal": jnp.clip(jax.random.uniform(splits[14], (REGIONS,), jnp.float32, 20.0, 60.0), 20.0, 60.0),
    }


step_dt = 0.2

def inverse_sinh(values):
    size_abs = jnp.abs(values)
    return jnp.sign(values) * jnp.log(size_abs + jnp.sqrt(size_abs * size_abs + 1.0))

def lower_diff(values, along, mask_cut):
    length = values.shape[along]
    beneath = jnp.concatenate([jnp.zeros_like(lax.slice_in_dim(values, 0, 1, axis=along)), lax.slice_in_dim(values, 0, length - 1, axis=along)], axis=along)
    if mask_cut is not None:
        beneath = beneath * mask_cut
    return values - beneath

def upper_diff(values, along, mask_cut):
    length = values.shape[along]
    overhead = jnp.concatenate([lax.slice_in_dim(values, 1, length, axis=along), jnp.zeros_like(lax.slice_in_dim(values, 0, 1, axis=along))], axis=along)
    if mask_cut is not None:
        overhead = overhead * mask_cut
    return overhead - values

def friction(minus_side, plus_side, minus_buoy, plus_buoy, prestress, fault_mask, region_ids, inverse_rate, slip_prev, region_a, region_normal):
    impedance = 1.0 / (step_dt * (minus_buoy + plus_buoy))
    jump_vec = plus_side - minus_side
    normal_part = impedance * jump_vec[0]
    locked_y = prestress[0] + impedance * jump_vec[1]
    locked_z = prestress[1] + impedance * jump_vec[2]
    magnitude = jnp.sqrt(locked_y * locked_y + locked_z * locked_z + 1.0)
    labels = jnp.arange(region_a.shape[0], dtype=jnp.int32)
    picked = (region_ids[None] == labels[:, None, None]).astype(minus_buoy.dtype)
    strength = lax.optimization_barrier(jnp.sum(picked * region_a[:, None, None], axis=0)) * lax.optimization_barrier(jnp.sum(picked * region_normal[:, None, None], axis=0))
    velocity_slip = slip_prev
    for turn in range(NEWTON):
        scaled = inverse_rate * velocity_slip
        residual = magnitude - impedance * velocity_slip - strength * inverse_sinh(scaled)
        tangent = -impedance - strength * inverse_rate / jnp.sqrt(1.0 + scaled * scaled)
        velocity_slip = velocity_slip - residual / tangent
    velocity_slip = velocity_slip * fault_mask.astype(minus_buoy.dtype)
    retained = 1.0 - impedance * velocity_slip / magnitude
    traction = jnp.stack([normal_part, retained * locked_y - prestress[0], retained * locked_z - prestress[1]])
    return (traction, velocity_slip)

def one_step(velocity, stress, buoyancy, stiff_xx, stiff_xz, stiff_zz, shear_vert, shear_horiz, prestress, fault_mask, region_ids, inverse_rate, slip_prev, region_a, region_normal):
    middle = velocity.shape[2] // 2
    normal_index = jnp.arange(velocity.shape[2], dtype=jnp.int32)[None, :, None]
    cut_lower = (normal_index != middle).astype(velocity.dtype)
    cut_upper = (normal_index != middle - 1).astype(velocity.dtype)
    stress_xx, stress_yy, stress_zz, stress_yz, stress_xz, stress_xy = stress
    trial_x = velocity[0] + step_dt * buoyancy * (lower_diff(stress_xx, 1, cut_lower) + lower_diff(stress_xy, 0, None) + lower_diff(stress_xz, 2, None))
    trial_y = velocity[1] + step_dt * buoyancy * (lower_diff(stress_xy, 1, cut_lower) + lower_diff(stress_yy, 0, None) + lower_diff(stress_yz, 2, None))
    trial_z = velocity[2] + step_dt * buoyancy * (lower_diff(stress_xz, 1, cut_lower) + lower_diff(stress_yz, 0, None) + lower_diff(stress_zz, 2, None))
    trial = jnp.stack([trial_x, trial_y, trial_z])
    minus_buoy = buoyancy[:, middle - 1, :]
    plus_buoy = buoyancy[:, middle, :]
    traction, slip_rate = friction(trial[:, :, middle - 1, :], trial[:, :, middle, :], minus_buoy, plus_buoy, prestress, fault_mask, region_ids, inverse_rate, slip_prev, region_a, region_normal)
    moved = trial.at[:, :, middle - 1, :].add(step_dt * minus_buoy * traction)
    moved = moved.at[:, :, middle, :].add(-(step_dt * plus_buoy * traction))
    moved_x, moved_y, moved_z = moved
    strain_xx = upper_diff(moved_x, 1, cut_upper)
    strain_yy = upper_diff(moved_y, 0, None)
    strain_zz = upper_diff(moved_z, 2, None)
    lame = stiff_xx - 2.0 * shear_horiz
    new_xx = stress_xx + step_dt * (stiff_xx * strain_xx + lame * strain_yy + stiff_xz * strain_zz)
    new_yy = stress_yy + step_dt * (lame * strain_xx + stiff_xx * strain_yy + stiff_xz * strain_zz)
    new_zz = stress_zz + step_dt * (stiff_xz * (strain_xx + strain_yy) + stiff_zz * strain_zz)
    new_yz = stress_yz + step_dt * shear_vert * (upper_diff(moved_y, 2, None) + upper_diff(moved_z, 0, None))
    new_xz = stress_xz + step_dt * shear_vert * (upper_diff(moved_x, 2, None) + upper_diff(moved_z, 1, cut_upper))
    new_xy = stress_xy + step_dt * shear_horiz * (upper_diff(moved_x, 0, None) + upper_diff(moved_y, 1, cut_upper))
    return (moved, jnp.stack([new_xx, new_yy, new_zz, new_yz, new_xz, new_xy]), slip_rate)

def reference(velocity, stress, buoyancy, stiff_xx, stiff_xz, stiff_zz, shear_vert, shear_horiz, prestress, fault_mask, region_ids, inverse_rate, slip_prev, region_a, region_normal):
    slip_rate = slip_prev
    for count in range(STEPS):
        velocity, stress, slip_rate = one_step(velocity, stress, buoyancy, stiff_xx, stiff_xz, stiff_zz, shear_vert, shear_horiz, prestress, fault_mask, region_ids, inverse_rate, slip_rate, region_a, region_normal)
    return (velocity, stress, slip_rate)
```

```python
import functools

import jax
import jax.numpy as jnp
from jax import lax
from jax.experimental import pallas as pl
from jax.experimental.pallas import tpu as pltpu
from jax.sharding import PartitionSpec as P

STEPS = 3
NEWTON = 3
DT = 0.2
MESH = pl.DeviceIdType.MESH

S_ORDER = (0, 2, 4, 3, 1, 5)
XX, ZZ, XZ, YZ, YY, XY = range(6)
BUO, C11, C66, C13, C44, C33 = range(6)

PLANES = 8
ROWS = 128
TILES = 17
EXT = 8 * TILES
GHOST = slice(ROWS, EXT)


def kernel(
    vel_hbm, str_hbm, buo_hbm, c11_hbm, c13_hbm, c33_hbm, c44_hbm, c66_hbm,
    pre_hbm, mask_hbm, ids_hbm, inv_hbm, slip_hbm, reg_a_hbm, reg_n_hbm,
    vel_out, str_out, slip_out,
    S, V, C, VN, VP, PK, ZN, ZM, ZD1, ZD2, PI, ZI, UN, UM, UO, UD1, UD2, SG, CG,
    FB, SE, VE, CE, pre, mask, ids, inv, slip, strength, reg_a, reg_n,
    lsem, ssem, rsem,
):
    f32 = jnp.float32
    ngy, ngz = lax.axis_size("gy"), lax.axis_size("gz")
    gx, gy, gz = lax.axis_index("gx"), lax.axis_index("gy"), lax.axis_index("gz")
    is_minus = gx == 0
    lane = lax.broadcasted_iota(jnp.int32, (8, 128), 1)
    sub = lax.broadcasted_iota(jnp.int32, (8, 128), 0)
    edge = (1 - gx) * (ROWS - 8)
    own_f = (1 - gx) * (ROWS - 1)
    other_f = ROWS + gx * 7

    up_y, dn_y, up_z, dn_z = gy < ngy - 1, gy > 0, gz < ngz - 1, gz > 0

    def at(dx, dy, dz):
        return (
            gx if dx == 0 else 1 - gx,
            jnp.clip(gy + dy, 0, ngy - 1),
            jnp.clip(gz + dz, 0, ngz - 1),
        )

    def exists(dy, dz):
        ok = gy >= 0
        if dy:
            ok = jnp.logical_and(ok, up_y if dy > 0 else dn_y)
        if dz:
            ok = jnp.logical_and(ok, up_z if dz > 0 else dn_z)
        return ok

    barrier = pltpu.get_barrier_semaphore()
    around = [
        (0, 1, 0), (0, -1, 0), (0, 0, 1), (0, 0, -1), (0, -1, 1), (0, 1, -1),
        (1, 0, 0), (1, 1, 0), (1, -1, 0), (1, 0, 1), (1, 0, -1),
    ]
    count = jnp.int32(0)
    for dx, dy, dz in around:
        ok = exists(dy, dz)
        count = count + ok.astype(jnp.int32)

        @pl.when(ok)
        def _():
            pl.semaphore_signal(barrier, inc=1, device_id=at(dx, dy, dz), device_id_type=MESH)

    loads = {}

    def load(name, src, dst):
        copy = pltpu.make_async_copy(src, dst, lsem.at[len(loads)])
        copy.start()
        loads[name] = copy

    own = pl.ds(0, ROWS)
    edge_rows = pl.ds(pl.multiple_of(edge, 8), 8)
    for i in range(6):
        load(("se", i), str_hbm.at[S_ORDER[i], :, edge_rows], SE.at[i])
    load("ve", vel_hbm.at[:, :, edge_rows], VE)
    coefficients = ((BUO, buo_hbm), (C11, c11_hbm), (C66, c66_hbm), (C13, c13_hbm), (C44, c44_hbm), (C33, c33_hbm))
    for i, ref in coefficients:
        load(("ce", i), ref.at[:, edge_rows], CE.at[i])
    for i in (YZ, YY, XY):
        load(("s7", i), str_hbm.at[S_ORDER[i], PLANES - 1], S.at[i, PLANES, own])
    for i in (ZZ, XZ):
        load(("s", i), str_hbm.at[S_ORDER[i]], S.at[i, pl.ds(1, PLANES), own])
    for i in (YZ, YY, XY):
        load(("s", i), str_hbm.at[S_ORDER[i], pl.ds(0, PLANES - 1)], S.at[i, pl.ds(1, PLANES - 1), own])
    load(("s", XX), str_hbm.at[S_ORDER[XX]], S.at[XX, pl.ds(1, PLANES), own])
    load("v", vel_hbm, V.at[:, :, own])
    for i, ref in coefficients:
        load(i, ref, C.at[i, pl.ds(1, PLANES), own])
    load("pre", pre_hbm, pre)
    load("mask", mask_hbm, mask)
    load("ids", ids_hbm, ids)
    load("inv", inv_hbm, inv)
    load("slip", slip_hbm, slip)
    load("reg_a", reg_a_hbm, reg_a)
    load("reg_n", reg_n_hbm, reg_n)

    sent = {}

    def message(name, src, dst, dx, dy, dz):
        i = len(sent)
        copy = pltpu.make_async_remote_copy(
            src_ref=src, dst_ref=dst, send_sem=ssem.at[i], recv_sem=rsem.at[i],
            device_id=at(dx, dy, dz), device_id_type=MESH,
        )
        sent[name] = [copy, exists(dy, dz), exists(-dy, -dz), True]

        @pl.when(exists(dy, dz))
        def _():
            copy.start()

    def arrived(name):
        copy, _, source, _ = sent[name]

        @pl.when(source)
        def _():
            copy.wait_recv()

    def gone(name):
        copy, target, _, pending = sent[name]
        if pending:
            sent[name][3] = False

            @pl.when(target)
            def _():
                copy.wait_send()

    def rows(t):
        return pl.ds(8 * t, 8)

    def below(ref, lead, t):
        if t in (0, TILES - 1):
            return jnp.where(sub == 0, 0.0, pltpu.roll(ref[lead + (rows(t),)], 1, 0))
        return ref[lead + (pl.ds(8 * t - 1, 8),)]

    def above(ref, lead, t):
        if t in (TILES - 2, TILES - 1):
            return jnp.where(sub == 7, 0.0, pltpu.roll(ref[lead + (rows(t),)], 7, 0))
        return ref[lead + (pl.ds(8 * t + 1, 8),)]

    def pack(ref, lead, plane0, out, tiles):
        groups = (tiles + 1) // 2

        def body(c, accs):
            accs = list(accs)
            for y in range(PLANES):
                for t in range(tiles):
                    base = 64 * (t % 2) + 16 * c + 2 * y
                    moved = pltpu.roll(ref[lead + c, plane0 + y, rows(t)], base + 1, 1)
                    hit = jnp.logical_or(lane == base, lane == base + 1)
                    accs[t // 2] = jnp.where(hit, moved, accs[t // 2])
            return tuple(accs)

        accs = lax.fori_loop(0, 3, body, tuple(jnp.zeros((8, 128), f32) for _ in range(groups)))
        for g in range(groups):
            out[pl.ds(8 * g, 8)] = accs[g]
        return accs

    def unpack(src, dst):
        for t in range(TILES):
            tile = src[pl.ds(8 * (t // 2), 8)]
            dst[rows(t)] = tile if t % 2 == 0 else pltpu.roll(tile, 64, 1)

    def trial(y, tiles):
        back = lax.rem(128 - 2 * y, 128)

        def lower_dip(value, i, t):
            halo = pltpu.roll(SG[i, rows(t)], back, 1)
            return value - jnp.where(lane == 0, halo, pltpu.roll(value, 1, 1))

        for t in tiles:
            r = rows(t)
            sxx, szz, sxz, syz, syy, sxy = (S[i, y + 1, r] for i in range(6))
            scale = DT * C[BUO, y + 1, r]
            vx = V[0, y, r] + scale * (
                (sxx - below(S, (XX, y + 1), t)) + (sxy - S[XY, y, r]) + lower_dip(sxz, 1, t)
            )
            vy = V[1, y, r] + scale * (
                (sxy - below(S, (XY, y + 1), t)) + (syy - S[YY, y, r]) + lower_dip(syz, 2, t)
            )
            vz = V[2, y, r] + scale * (
                (sxz - below(S, (XZ, y + 1), t)) + (syz - S[YZ, y, r]) + lower_dip(szz, 0, t)
            )
            V[0, y, r] = vx
            V[1, y, r] = vy
            V[2, y, r] = vz

    def stress(p, here, here_lead, over, over_lead, halo, halo_y, ghost=False, last=False):
        def put(i, value):
            if last:
                str_out[S_ORDER[i], p - 1, r] = value
            else:
                S[i, p, r] = value

        for t in range(TILES - 1 if last else TILES):
            r = rows(t)

            def upper_dip(value, c):
                edge_column = pltpu.roll(halo[r], 126 - 16 * c - 2 * halo_y, 1)
                return jnp.where(lane == 127, edge_column, pltpu.roll(value, 127, 1)) - value

            vx, vy, vz = (here[here_lead(c) + (r,)] for c in range(3))
            ox, oy, oz = (over[over_lead(c) + (r,)] for c in range(3))
            exx = above(here, here_lead(0), t) - vx
            eyy = oy - vy
            ezz = upper_dip(vz, 2)
            c11, c66, c13, c44 = (C[i, p, r] for i in (C11, C66, C13, C44))
            lame = c11 - 2.0 * c66
            put(YY, S[YY, p, r] + DT * (lame * exx + c11 * eyy + c13 * ezz))
            put(YZ, S[YZ, p, r] + DT * c44 * (upper_dip(vy, 1) + (oz - vz)))
            put(XY, S[XY, p, r] + DT * c66 * ((ox - vx) + (above(here, here_lead(1), t) - vy)))
            if not ghost:
                put(XX, S[XX, p, r] + DT * (c11 * exx + lame * eyy + c13 * ezz))
                put(ZZ, S[ZZ, p, r] + DT * (c13 * (exx + eyy) + C[C33, p, r] * ezz))
                put(XZ, S[XZ, p, r] + DT * c44 * (
                    upper_dip(vx, 0) + (above(here, here_lead(2), t) - vz)
                ))

    def stress_own(k, y):
        stress(y + 1, V, lambda c: (c, y), V, lambda c: (c, y + 1), UN, y, last=k == STEPS - 1)

    def stress_last(k):
        stress(PLANES, V, lambda c: (c, PLANES - 1), VN, lambda c: (k, c), UN, PLANES - 1, last=k == STEPS - 1)

    def stress_ghost(k):
        stress(0, VP, lambda c: (k, c), V, lambda c: (c, 0), UD2, PLANES - 1, ghost=True)

    def column_ghost():
        for t in range(TILES):
            r = rows(t)

            def shifted(ref, by):
                return pltpu.roll(ref[r], by % 128, 1)

            def upper_rows(c):
                if t in (TILES - 2, TILES - 1):
                    return pltpu.roll(
                        jnp.where(sub == 7, 0.0, pltpu.roll(UM[r], 7, 0)), (-16 * c) % 128, 1
                    )
                return pltpu.roll(UM[pl.ds(8 * t + 1, 8)], (-16 * c) % 128, 1)

            def next_strike(value, c):
                corner = shifted(UD1, 14 - 16 * c)
                return jnp.where(lane == 14, corner, pltpu.roll(value, 126, 1))

            vx, vy, vz = UM[r], shifted(UM, -16), shifted(UM, -32)
            ox, oy, oz = shifted(UO, -1), shifted(UO, -17), shifted(UO, -33)
            exx = upper_rows(0) - vx
            eyy = next_strike(vy, 1) - vy
            ezz = oz - vz
            c13, c44, c33 = CG[0, r], CG[1, r], CG[2, r]
            SG[0, r] = SG[0, r] + DT * (c13 * (exx + eyy) + c33 * ezz)
            SG[1, r] = SG[1, r] + DT * c44 * ((ox - vx) + (upper_rows(2) - vz))
            SG[2, r] = SG[2, r] + DT * c44 * ((oy - vy) + (next_strike(vz, 2) - vz))

    def fault():
        for c in range(3):
            for y in range(PLANES):
                FB[c, pl.ds(y, 1)] = V[c, y, pl.ds(own_f, 1)]
                FB[3 + c, pl.ds(y, 1)] = V[c, y, pl.ds(other_f, 1)]
        own_v, other_v = [FB[c] for c in range(3)], [FB[3 + c] for c in range(3)]
        own_b, other_b = FB[6], FB[7]
        minus_b = jnp.where(is_minus, own_b, other_b)
        plus_b = jnp.where(is_minus, other_b, own_b)
        minus_v = [jnp.where(is_minus, a, b) for a, b in zip(own_v, other_v)]
        plus_v = [jnp.where(is_minus, b, a) for a, b in zip(own_v, other_v)]
        impedance = 1.0 / (DT * (minus_b + plus_b))
        jump = [b - a for a, b in zip(minus_v, plus_v)]
        locked_y = pre[0] + impedance * jump[1]
        locked_z = pre[1] + impedance * jump[2]
        magnitude = jnp.sqrt(locked_y * locked_y + locked_z * locked_z + 1.0)
        hold = strength[...]
        rate = inv[...]
        value = slip[...]
        for _ in range(NEWTON):
            scaled = rate * value
            size = jnp.abs(scaled)
            root = jnp.sqrt(size * size + 1.0)
            log = jnp.log(size + root)
            residual = magnitude - impedance * value - hold * jnp.where(scaled < 0.0, -log, log)
            tangent = -impedance - hold * rate / root
            value = value - residual / tangent
        value = value * mask[...].astype(f32)
        slip[...] = value
        retained = 1.0 - impedance * value / magnitude
        traction = [impedance * jump[0], retained * locked_y - pre[0], retained * locked_z - pre[1]]
        for c in range(3):
            minus_new = minus_v[c] + DT * minus_b * traction[c]
            plus_new = plus_v[c] - DT * plus_b * traction[c]
            FB[c] = jnp.where(is_minus, minus_new, plus_new)
            FB[3 + c] = jnp.where(is_minus, plus_new, minus_new)
        for c in range(3):
            for y in range(PLANES):
                V[c, y, pl.ds(own_f, 1)] = FB[c, pl.ds(y, 1)]
                V[c, y, pl.ds(other_f, 1)] = FB[3 + c, pl.ds(y, 1)]

    @pl.when(jnp.logical_not(up_y))
    def _():
        VN[...] = jnp.zeros(VN.shape, f32)
        ZD1[...] = jnp.zeros(ZD1.shape, f32)

    @pl.when(jnp.logical_not(dn_y))
    def _():
        S[pl.ds(YZ, 3), 0] = jnp.zeros((3, EXT, 128), f32)

    @pl.when(jnp.logical_not(up_z))
    def _():
        ZN[...] = jnp.zeros(ZN.shape, f32)
        ZD2[...] = jnp.zeros(ZD2.shape, f32)

    @pl.when(jnp.logical_not(dn_z))
    def _():
        SG[...] = jnp.zeros(SG.shape, f32)

    ghost_rows = pl.ds(ROWS, 8)
    every = pl.ds(1, PLANES)
    strike = pl.ds(YZ, 3)
    strike_c = pl.ds(C11, 4)
    rest = pl.ds(C11, 5)
    for i in (YZ, YY, XY):
        loads["s7", i].wait()
    for i in range(6):
        loads["se", i].wait()
    loads["ve"].wait()
    for i in range(6):
        loads["ce", i].wait()
    pl.semaphore_wait(barrier, count)
    message("y0", S.at[strike, PLANES, own], S.at[strike, 0, own], 0, 1, 0)
    message("xy0", SE.at[strike, PLANES - 1], S.at[strike, 0, ghost_rows], 1, 1, 0)
    message("x0", SE, S.at[:, every, ghost_rows], 1, 0, 0)
    message("xv", VE, V.at[:, :, ghost_rows], 1, 0, 0)
    message("xb", CE.at[BUO], C.at[BUO, every, ghost_rows], 1, 0, 0)
    for i in (ZZ, XZ, YZ, YY, XY, XX):
        loads["s", i].wait()
    accs = pack(S, ZZ, 1, PI.at[0], 16)
    message("z0", PI.at[0, pl.ds(0, 64)], ZI.at[0, pl.ds(0, 64)], 0, 0, 1)
    PI[0, pl.ds(64, 8)] = jnp.where(is_minus, pltpu.roll(accs[7], 64, 1), accs[0])
    message("xz0", PI.at[0, pl.ds(64, 8)], ZI.at[0, pl.ds(64, 8)], 1, 0, 1)
    loads["v"].wait()
    for i in range(6):
        loads[i].wait()
    message("xc", CE.at[rest], C.at[rest, every, ghost_rows], 1, 0, 0)
    message("yc", C.at[strike_c, PLANES, own], C.at[strike_c, 0, own], 0, 1, 0)
    message("xyc", CE.at[strike_c, PLANES - 1], C.at[strike_c, 0, ghost_rows], 1, 1, 0)
    accs = pack(C, C13, 1, PI.at[1], 16)
    message("zc", PI.at[1, pl.ds(0, 64)], ZI.at[1, pl.ds(0, 64)], 0, 0, 1)
    PI[1, pl.ds(64, 8)] = jnp.where(is_minus, pltpu.roll(accs[7], 64, 1), accs[0])
    message("xzc", PI.at[1, pl.ds(64, 8)], ZI.at[1, pl.ds(64, 8)], 1, 0, 1)

    for name in ("pre", "mask", "ids", "inv", "slip", "reg_a", "reg_n"):
        loads[name].wait()
    number = ids[...]
    picked_a = jnp.zeros((8, 128), f32)
    picked_n = jnp.zeros((8, 128), f32)
    for i in range(8):
        picked_a = jnp.where(number == i, reg_a[i], picked_a)
        picked_n = jnp.where(number == i, reg_n[i], picked_n)
    strength[...] = picked_a * picked_n

    def columns(src, dst):
        for t in range(TILES):
            tile = src[pl.ds(8 * (t // 2), 8)]
            for c in range(3):
                shift = (-16 * c - 64 * (t % 2)) % 128
                dst[c, rows(t)] = pltpu.roll(tile, shift, 1) if shift else tile

    arrived("z0")
    arrived("xz0")

    @pl.when(dn_z)
    def _():
        columns(ZI.at[0], SG)

    own_tiles = range(TILES - 1)
    all_tiles = range(TILES)

    def planes(first, last, body):
        def step(y, carry):
            body(y)
            return carry

        lax.fori_loop(first, last, step, 0)

    planes(1, PLANES, lambda y: trial(y, own_tiles))
    arrived("x0")
    arrived("xv")
    arrived("xb")
    arrived("xy0")
    for y in range(PLANES):
        FB[6, pl.ds(y, 1)] = C[BUO, y + 1, pl.ds(own_f, 1)]
        FB[7, pl.ds(y, 1)] = C[BUO, y + 1, pl.ds(other_f, 1)]
    planes(0, PLANES, lambda y: trial(y, [TILES - 1]))
    arrived("y0")
    planes(0, 1, lambda y: trial(y, own_tiles))

    for k in range(STEPS):
        last = k == STEPS - 1
        fault()
        message(("yb", k), V.at[:, 0], VN.at[k], 0, -1, 0)
        if not last:
            message(("yf", k), V.at[:, PLANES - 1], VP.at[k], 0, 1, 0)
        else:
            slip_out[...] = slip[...]

            def copy_plane(y):
                for c in range(3):
                    vel_out[c, y] = V[c, y, own]

            planes(0, PLANES, copy_plane)
        pack(V, 0, 0, PK.at[k], TILES)
        message(("zb", k), PK.at[k], ZN.at[k], 0, 0, -1)
        if not last:
            message(("zf", k), PK.at[k], ZM.at[k], 0, 0, 1)
            message(("d1", k), PK.at[k], ZD1.at[k], 0, -1, 1)
            message(("d2", k), PK.at[k], ZD2.at[k], 0, 1, -1)
        if k == 0:
            arrived("zc")
            arrived("xzc")

            @pl.when(dn_z)
            def _():
                columns(ZI.at[1], CG)

            arrived("xc")
            gone("y0")
        arrived(("zb", k))
        unpack(ZN.at[k], UN)
        planes(0, PLANES - 1, functools.partial(stress_own, k))
        if last:
            arrived(("yb", k))
            planes(0, 1, lambda y: stress_last(k))
            break
        arrived(("zf", k))
        arrived(("d1", k))

        @pl.when(dn_z)
        def _():
            unpack(ZM.at[k], UM)
            unpack(ZD1.at[k], UD1)
            unpack(PK.at[k], UO)
            column_ghost()

        planes(1, PLANES - 1, lambda y: trial(y, all_tiles))
        if k == 0:
            arrived("yc")
            arrived("xyc")
        arrived(("d2", k))
        arrived(("yf", k))

        @pl.when(dn_y)
        def _():
            unpack(ZD2.at[k], UD2)
            stress_ghost(k)

        arrived(("yb", k))
        gone(("yb", k))
        gone(("yf", k))
        planes(0, 1, lambda y: stress_last(k))
        planes(0, 2, lambda i: trial((PLANES - 1) * i, all_tiles))

    for name in list(sent):
        gone(name)


def local(
    velocity, stress, buoyancy, stiff_xx, stiff_xz, stiff_zz, shear_vert, shear_horiz,
    prestress, fault_mask, region_ids, inverse_rate, slip_prev, region_a, region_normal,
):
    f32 = jnp.float32
    hbm = pl.BlockSpec(memory_space=pltpu.HBM)
    vmem = pl.BlockSpec(memory_space=pltpu.VMEM)
    tile = pltpu.VMEM((8, 128), f32)
    plane = (EXT, 128)
    packed = (72, 128)
    large = [
        pltpu.with_memory_space_constraint(x, pltpu.HBM)
        for x in (
            velocity, stress, buoyancy, stiff_xx, stiff_xz, stiff_zz, shear_vert, shear_horiz,
            prestress, fault_mask, region_ids, inverse_rate, slip_prev, region_a, region_normal,
        )
    ]
    return pl.pallas_call(
        kernel,
        out_shape=(
            jax.ShapeDtypeStruct(velocity.shape, f32),
            jax.ShapeDtypeStruct(stress.shape, f32),
            jax.ShapeDtypeStruct(slip_prev.shape, f32),
        ),
        in_specs=[hbm] * 15,
        out_specs=(vmem, vmem, vmem),
        scratch_shapes=[
            pltpu.VMEM((6, PLANES + 1) + plane, f32),
            pltpu.VMEM((3, PLANES) + plane, f32),
            pltpu.VMEM((6, PLANES + 1) + plane, f32),
            pltpu.VMEM((STEPS, 3) + plane, f32),
            pltpu.VMEM((STEPS - 1, 3) + plane, f32),
            pltpu.VMEM((STEPS,) + packed, f32),
            pltpu.VMEM((STEPS,) + packed, f32),
            pltpu.VMEM((STEPS - 1,) + packed, f32),
            pltpu.VMEM((STEPS - 1,) + packed, f32),
            pltpu.VMEM((STEPS - 1,) + packed, f32),
            pltpu.VMEM((2,) + packed, f32),
            pltpu.VMEM((2,) + packed, f32),
            pltpu.VMEM(plane, f32),
            pltpu.VMEM(plane, f32),
            pltpu.VMEM(plane, f32),
            pltpu.VMEM(plane, f32),
            pltpu.VMEM(plane, f32),
            pltpu.VMEM((3,) + plane, f32),
            pltpu.VMEM((3,) + plane, f32),
            pltpu.VMEM((8, 8, 128), f32),
            pltpu.VMEM((6, PLANES, 8, 128), f32),
            pltpu.VMEM((3, PLANES, 8, 128), f32),
            pltpu.VMEM((6, PLANES, 8, 128), f32),
            pltpu.VMEM((2, 8, 128), f32),
            pltpu.VMEM((8, 128), jnp.int32),
            pltpu.VMEM((8, 128), jnp.int32),
            tile,
            tile,
            tile,
            pltpu.SMEM((8,), f32),
            pltpu.SMEM((8,), f32),
            pltpu.SemaphoreType.DMA((40,)),
            pltpu.SemaphoreType.DMA((32,)),
            pltpu.SemaphoreType.DMA((32,)),
        ],
        compiler_params=pltpu.CompilerParams(
            collective_id=0, has_side_effects=True, vmem_limit_bytes=40 * 1024 * 1024
        ),
        name="rupture",
    )(*large)


def solution(mesh):
    cell, fault_tile = P("gy", "gx", "gz"), P("gy", "gz")
    field = P(None, "gy", "gx", "gz")
    in_specs = (field, field) + (cell,) * 6 + (P(None, "gy", "gz"),) + (fault_tile,) * 4 + (P(), P())
    out_specs = (field, field, fault_tile)
    return jax.shard_map(local, mesh=mesh, in_specs=in_specs, out_specs=out_specs, check_vma=False)
```

```python
import functools

import jax
import jax.numpy as jnp
from jax import lax
from jax.experimental import pallas as pl
from jax.experimental.pallas import tpu as pltpu
from jax.sharding import PartitionSpec as P

STEPS = 3
NEWTON = 3
DT = 0.2
MESH = pl.DeviceIdType.MESH

S_ORDER = (0, 2, 4, 3, 1, 5)
XX, ZZ, XZ, YZ, YY, XY = range(6)
BUO, C11, C66, C13, C44, C33 = range(6)

PLANES = 8
ROWS = 128
TILES = 17
EXT = 8 * TILES
GHOST = slice(ROWS, EXT)


def kernel(
    vel_hbm, str_hbm, buo_hbm, c11_hbm, c13_hbm, c33_hbm, c44_hbm, c66_hbm,
    pre_hbm, mask_hbm, ids_hbm, inv_hbm, slip_hbm, reg_a_hbm, reg_n_hbm,
    vel_out, str_out, slip_out,
    S, V, C, VN, VP, PK, ZN, ZM, GP, CK, ZD1, ZD2, PI, ZI, UN, UM, UO, SG, CG,
    FB, SE, VE, CE, XS, XR, pre, mask, ids, inv, slip, strength, reg_a, reg_n,
    lsem, ssem, rsem,
):
    f32 = jnp.float32
    ngy, ngz = lax.axis_size("gy"), lax.axis_size("gz")
    gx, gy, gz = lax.axis_index("gx"), lax.axis_index("gy"), lax.axis_index("gz")
    is_minus = gx == 0
    lane = lax.broadcasted_iota(jnp.int32, (8, 128), 1)
    sub = lax.broadcasted_iota(jnp.int32, (8, 128), 0)
    edge = (1 - gx) * (ROWS - 8)
    own_f = (1 - gx) * (ROWS - 1)
    other_f = ROWS + gx * 7

    up_y, dn_y, up_z, dn_z = gy < ngy - 1, gy > 0, gz < ngz - 1, gz > 0

    def at(dx, dy, dz):
        return (
            gx if dx == 0 else 1 - gx,
            jnp.clip(gy + dy, 0, ngy - 1),
            jnp.clip(gz + dz, 0, ngz - 1),
        )

    def exists(dy, dz):
        ok = gy >= 0
        if dy:
            ok = jnp.logical_and(ok, up_y if dy > 0 else dn_y)
        if dz:
            ok = jnp.logical_and(ok, up_z if dz > 0 else dn_z)
        return ok

    barrier = pltpu.get_barrier_semaphore()
    around = [
        (0, 1, 0), (0, -1, 0), (0, 0, 1), (0, 0, -1), (0, -1, 1), (0, 1, -1),
        (1, 0, 0), (1, 1, 0), (1, -1, 0), (1, 0, 1), (1, 0, -1),
    ]
    count = jnp.int32(0)
    for dx, dy, dz in around:
        ok = exists(dy, dz)
        count = count + ok.astype(jnp.int32)

        @pl.when(ok)
        def _():
            pl.semaphore_signal(barrier, inc=1, device_id=at(dx, dy, dz), device_id_type=MESH)

    loads = {}

    def load(name, src, dst):
        copy = pltpu.make_async_copy(src, dst, lsem.at[len(loads)])
        copy.start()
        loads[name] = copy

    own = pl.ds(0, ROWS)
    edge_rows = pl.ds(pl.multiple_of(edge, 8), 8)
    for i in range(6):
        load(("se", i), str_hbm.at[S_ORDER[i], :, edge_rows], SE.at[i])
    load("ve", vel_hbm.at[:, :, edge_rows], VE)
    coefficients = ((BUO, buo_hbm), (C11, c11_hbm), (C66, c66_hbm), (C13, c13_hbm), (C44, c44_hbm), (C33, c33_hbm))
    for i, ref in coefficients:
        load(("ce", i), ref.at[:, edge_rows], CE.at[i])
    for i in (YZ, YY, XY):
        load(("s7", i), str_hbm.at[S_ORDER[i], PLANES - 1], S.at[i, PLANES, own])
    for i in (ZZ, XZ):
        load(("s", i), str_hbm.at[S_ORDER[i]], S.at[i, pl.ds(1, PLANES), own])
    for i in (YZ, YY, XY):
        load(("s", i), str_hbm.at[S_ORDER[i], pl.ds(0, PLANES - 1)], S.at[i, pl.ds(1, PLANES - 1), own])
    load(("s", XX), str_hbm.at[S_ORDER[XX]], S.at[XX, pl.ds(1, PLANES), own])
    load("v", vel_hbm, V.at[:, :, own])
    for i, ref in coefficients:
        load(i, ref, C.at[i, pl.ds(1, PLANES), own])
    load("pre", pre_hbm, pre)
    load("mask", mask_hbm, mask)
    load("ids", ids_hbm, ids)
    load("inv", inv_hbm, inv)
    load("slip", slip_hbm, slip)
    load("reg_a", reg_a_hbm, reg_a)
    load("reg_n", reg_n_hbm, reg_n)

    sent = {}

    def message(name, src, dst, dx, dy, dz):
        i = len(sent)
        copy = pltpu.make_async_remote_copy(
            src_ref=src, dst_ref=dst, send_sem=ssem.at[i], recv_sem=rsem.at[i],
            device_id=at(dx, dy, dz), device_id_type=MESH,
        )
        sent[name] = [copy, exists(dy, dz), exists(-dy, -dz), True]

        @pl.when(exists(dy, dz))
        def _():
            copy.start()

    def arrived(name):
        copy, _, source, _ = sent[name]

        @pl.when(source)
        def _():
            copy.wait_recv()

    def gone(name):
        copy, target, _, pending = sent[name]
        if pending:
            sent[name][3] = False

            @pl.when(target)
            def _():
                copy.wait_send()

    def rows(t):
        return pl.ds(8 * t, 8)

    def below(ref, lead, t):
        if t in (0, TILES - 1):
            return jnp.where(sub == 0, 0.0, pltpu.roll(ref[lead + (rows(t),)], 1, 0))
        return ref[lead + (pl.ds(8 * t - 1, 8),)]

    def above(ref, lead, t):
        if t in (TILES - 2, TILES - 1):
            return jnp.where(sub == 7, 0.0, pltpu.roll(ref[lead + (rows(t),)], 7, 0))
        return ref[lead + (pl.ds(8 * t + 1, 8),)]

    def pack(ref, lead, plane0, out, tiles, pick=lambda y, t: True):
        groups = (tiles + 1) // 2

        def body(c, accs):
            accs = list(accs)
            for y in range(PLANES):
                for t in range(tiles):
                    if not pick(y, t):
                        continue
                    base = 64 * (t % 2) + 16 * c + 2 * y
                    moved = pltpu.roll(ref[lead + c, plane0 + y, rows(t)], base + 1, 1)
                    hit = jnp.logical_or(lane == base, lane == base + 1)
                    accs[t // 2] = jnp.where(hit, moved, accs[t // 2])
            return tuple(accs)

        accs = lax.fori_loop(0, 3, body, tuple(jnp.zeros((8, 128), f32) for _ in range(groups)))
        for g in range(groups):
            out[pl.ds(8 * g, 8)] = accs[g]
        return accs

    FAULT = (0, TILES - 2, TILES - 1)
    INNER = range(1, TILES - 2)

    def early(y, t):
        return 0 < y < PLANES - 1 and t in INNER

    def merge(src, dst):
        strike_index = lax.rem(lane, 16) // 2
        outer = jnp.logical_or(strike_index == 0, strike_index == PLANES - 1)
        for g in range((TILES + 1) // 2):
            late = outer
            if 2 * g in FAULT:
                late = jnp.logical_or(late, lane < 64)
            if 2 * g + 1 in FAULT:
                late = jnp.logical_or(late, lane >= 64)
            tile = jnp.where(late, src[1, pl.ds(8 * g, 8)], src[0, pl.ds(8 * g, 8)])
            dst[rows(2 * g)] = tile
            if 2 * g + 1 < TILES:
                dst[rows(2 * g + 1)] = pltpu.roll(tile, 64, 1)

    def unpack(src, dst):
        for t in range(TILES):
            tile = src[pl.ds(8 * (t // 2), 8)]
            dst[rows(t)] = tile if t % 2 == 0 else pltpu.roll(tile, 64, 1)

    def corners(k):
        accs = [jnp.zeros((8, 128), f32), jnp.zeros((8, 128), f32)]
        for t in range(TILES):
            for c in range(3):
                base = 8 * (t % 16) + 2 * c
                both = jnp.where(lane == 127, V[c, 0, rows(t)], V[c, PLANES - 1, rows(t)])
                hit = jnp.logical_or(lane == base, lane == base + 1)
                accs[t // 16] = jnp.where(hit, pltpu.roll(both, base + 1, 1), accs[t // 16])
        for g in range(2):
            CK[k, pl.ds(8 * g, 8)] = accs[g]

    def corner_of(ref, k, t, c, by):
        return pltpu.roll(ref[k, pl.ds(8 * (t // 16), 8)], (by - 8 * (t % 16) - 2 * c) % 128, 1)

    def trial(y, tiles):
        back = (128 - 2 * y) % 128 if isinstance(y, int) else lax.rem(128 - 2 * y, 128)

        def lower_dip(value, i, t):
            halo = SG[i, rows(t)]
            if not isinstance(back, int) or back:
                halo = pltpu.roll(halo, back, 1)
            return value - jnp.where(lane == 0, halo, pltpu.roll(value, 1, 1))

        for t in tiles:
            r = rows(t)
            sxx, szz, sxz, syz, syy, sxy = (S[i, y + 1, r] for i in range(6))
            scale = DT * C[BUO, y + 1, r]
            vx = V[0, y, r] + scale * (
                (sxx - below(S, (XX, y + 1), t)) + (sxy - S[XY, y, r]) + lower_dip(sxz, 1, t)
            )
            vy = V[1, y, r] + scale * (
                (sxy - below(S, (XY, y + 1), t)) + (syy - S[YY, y, r]) + lower_dip(syz, 2, t)
            )
            vz = V[2, y, r] + scale * (
                (sxz - below(S, (XZ, y + 1), t)) + (syz - S[YZ, y, r]) + lower_dip(szz, 0, t)
            )
            V[0, y, r] = vx
            V[1, y, r] = vy
            V[2, y, r] = vz

    def stress(p, here, here_lead, over, over_lead, halo, ghost=False, last=False, tiles=range(TILES)):
        def put(i, value):
            if ghost:
                S[i, p, r] = jnp.where(dn_y, value, S[i, p, r])
            elif last:
                str_out[S_ORDER[i], p - 1, r] = value
            else:
                S[i, p, r] = value

        for t in tiles:
            if last and t == TILES - 1:
                continue
            r = rows(t)

            def upper_dip(value, c):
                return jnp.where(lane == 127, halo(c, t), pltpu.roll(value, 127, 1)) - value

            vx, vy, vz = (here[here_lead(c) + (r,)] for c in range(3))
            ox, oy, oz = (over[over_lead(c) + (r,)] for c in range(3))
            exx = above(here, here_lead(0), t) - vx
            eyy = oy - vy
            ezz = upper_dip(vz, 2)
            c11, c66, c13, c44 = (C[i, p, r] for i in (C11, C66, C13, C44))
            lame = c11 - 2.0 * c66
            put(YY, S[YY, p, r] + DT * (lame * exx + c11 * eyy + c13 * ezz))
            put(YZ, S[YZ, p, r] + DT * c44 * (upper_dip(vy, 1) + (oz - vz)))
            put(XY, S[XY, p, r] + DT * c66 * ((ox - vx) + (above(here, here_lead(1), t) - vy)))
            if not ghost:
                put(XX, S[XX, p, r] + DT * (c11 * exx + lame * eyy + c13 * ezz))
                put(ZZ, S[ZZ, p, r] + DT * (c13 * (exx + eyy) + C[C33, p, r] * ezz))
                put(XZ, S[XZ, p, r] + DT * c44 * (
                    upper_dip(vx, 0) + (above(here, here_lead(2), t) - vz)
                ))

    def next_dip(y):
        return lambda c, t: pltpu.roll(UN[rows(t)], 126 - 16 * c - 2 * y, 1)

    def stress_own(k, tiles, y):
        stress(
            y + 1, V, lambda c: (c, y), V, lambda c: (c, y + 1), next_dip(y),
            last=k == STEPS - 1, tiles=tiles,
        )

    def stress_last(k):
        stress(PLANES, V, lambda c: (c, PLANES - 1), VN, lambda c: (k, c), next_dip(PLANES - 1), last=k == STEPS - 1)

    def stress_ghost(k):
        stress(0, VP, lambda c: (k, c), V, lambda c: (c, 0), lambda c, t: corner_of(ZD2, k, t, c, 126), ghost=True)

    def column_ghost():
        for t in range(TILES):
            r = rows(t)

            def shifted(ref, by):
                return pltpu.roll(ref[r], by % 128, 1)

            def upper_rows(c):
                if t in (TILES - 2, TILES - 1):
                    return pltpu.roll(
                        jnp.where(sub == 7, 0.0, pltpu.roll(UM[r], 7, 0)), (-16 * c) % 128, 1
                    )
                return pltpu.roll(UM[pl.ds(8 * t + 1, 8)], (-16 * c) % 128, 1)

            vx, vy, vz = UM[r], shifted(UM, -16), shifted(UM, -32)
            ox, oy, oz = shifted(UO, -1), shifted(UO, -17), shifted(UO, -33)
            exx = upper_rows(0) - vx
            eyy = pltpu.roll(vy, 126, 1) - vy
            ezz = oz - vz
            c13, c44, c33 = CG[0, r], CG[1, r], CG[2, r]
            zz = SG[0, r] + DT * (c13 * (exx + eyy) + c33 * ezz)
            yz = SG[2, r] + DT * c44 * ((oy - vy) + (pltpu.roll(vz, 126, 1) - vz))
            SG[0, r] = jnp.where(lane == 14, SG[0, r], zz)
            SG[1, r] = SG[1, r] + DT * c44 * ((ox - vx) + (upper_rows(2) - vz))
            SG[2, r] = jnp.where(lane == 14, SG[2, r], yz)
            for i, value in enumerate((exx, vy, ezz, oy - vy, vz)):
                GP[i, r] = value

    def column_corner(k):
        here = jnp.logical_and(lane == 14, dn_z)
        for t in range(TILES):
            r = rows(t)
            exx, vy, ezz, oy_vy, vz = (GP[i, r] for i in range(5))
            eyy = corner_of(ZD1, k, t, 1, 14) - vy
            c13, c44, c33 = CG[0, r], CG[1, r], CG[2, r]
            zz = SG[0, r] + DT * (c13 * (exx + eyy) + c33 * ezz)
            yz = SG[2, r] + DT * c44 * (oy_vy + (corner_of(ZD1, k, t, 2, 14) - vz))
            SG[0, r] = jnp.where(here, zz, SG[0, r])
            SG[2, r] = jnp.where(here, yz, SG[2, r])

    def fault():
        for c in range(3):
            for y in range(PLANES):
                FB[c, pl.ds(y, 1)] = V[c, y, pl.ds(own_f, 1)]
                FB[3 + c, pl.ds(y, 1)] = V[c, y, pl.ds(other_f, 1)]
        own_v, other_v = [FB[c] for c in range(3)], [FB[3 + c] for c in range(3)]
        own_b, other_b = FB[6], FB[7]
        minus_b = jnp.where(is_minus, own_b, other_b)
        plus_b = jnp.where(is_minus, other_b, own_b)
        minus_v = [jnp.where(is_minus, a, b) for a, b in zip(own_v, other_v)]
        plus_v = [jnp.where(is_minus, b, a) for a, b in zip(own_v, other_v)]
        impedance = 1.0 / (DT * (minus_b + plus_b))
        jump = [b - a for a, b in zip(minus_v, plus_v)]
        locked_y = pre[0] + impedance * jump[1]
        locked_z = pre[1] + impedance * jump[2]
        magnitude = jnp.sqrt(locked_y * locked_y + locked_z * locked_z + 1.0)
        hold = strength[...]
        rate = inv[...]
        value = slip[...]
        for _ in range(NEWTON):
            scaled = rate * value
            size = jnp.abs(scaled)
            root = jnp.sqrt(size * size + 1.0)
            log = jnp.log(size + root)
            residual = magnitude - impedance * value - hold * jnp.where(scaled < 0.0, -log, log)
            tangent = -impedance - hold * rate / root
            value = value - residual / tangent
        value = value * mask[...].astype(f32)
        slip[...] = value
        retained = 1.0 - impedance * value / magnitude
        traction = [impedance * jump[0], retained * locked_y - pre[0], retained * locked_z - pre[1]]
        for c in range(3):
            minus_new = minus_v[c] + DT * minus_b * traction[c]
            plus_new = plus_v[c] - DT * plus_b * traction[c]
            FB[c] = jnp.where(is_minus, minus_new, plus_new)
            FB[3 + c] = jnp.where(is_minus, plus_new, minus_new)
        for c in range(3):
            for y in range(PLANES):
                V[c, y, pl.ds(own_f, 1)] = FB[c, pl.ds(y, 1)]
                V[c, y, pl.ds(other_f, 1)] = FB[3 + c, pl.ds(y, 1)]

    @pl.when(jnp.logical_not(up_y))
    def _():
        VN[...] = jnp.zeros(VN.shape, f32)
        ZD1[...] = jnp.zeros(ZD1.shape, f32)

    @pl.when(jnp.logical_not(dn_y))
    def _():
        S[pl.ds(YZ, 3), 0] = jnp.zeros((3, EXT, 128), f32)

    @pl.when(jnp.logical_not(up_z))
    def _():
        ZN[...] = jnp.zeros(ZN.shape, f32)
        ZD2[...] = jnp.zeros(ZD2.shape, f32)

    @pl.when(jnp.logical_not(dn_z))
    def _():
        SG[...] = jnp.zeros(SG.shape, f32)

    ghost_rows = pl.ds(ROWS, 8)
    strike = pl.ds(YZ, 3)
    strike_c = pl.ds(C11, 4)
    for i in (YZ, YY, XY):
        loads["s7", i].wait()
    for i in range(6):
        loads["se", i].wait()
    loads["ve"].wait()
    for i in range(6):
        loads["ce", i].wait()
    fields = [(SE, S, i, 1) for i in range(6)] + [(VE, V, i, 0) for i in range(3)]
    fields += [(CE, C, i, 1) for i in range(6)]
    for n, (src, _, i, _) in enumerate(fields):
        for q in range(PLANES // 2):
            first, second = src[i, 2 * q], src[i, 2 * q + 1]
            low = jnp.where(is_minus, pltpu.roll(first, 4, 0), first)
            high = jnp.where(is_minus, second, pltpu.roll(second, 4, 0))
            XS[n, q] = jnp.where(sub < 4, low, high)

    def spread(n):
        _, dst, i, base = fields[n]
        for q in range(PLANES // 2):
            value = XR[n, q]
            moved = pltpu.roll(value, 4, 0)
            dst[i, base + 2 * q, ghost_rows] = jnp.where(is_minus, value, moved)
            dst[i, base + 2 * q + 1, ghost_rows] = jnp.where(is_minus, moved, value)

    for i in (ZZ, XZ, YZ, YY, XY, XX):
        loads["s", i].wait()
    accs = pack(S, ZZ, 1, PI.at[0], 16)
    PI[0, pl.ds(64, 8)] = jnp.where(is_minus, pltpu.roll(accs[7], 64, 1), accs[0])
    pl.semaphore_wait(barrier, count)
    message("y0", S.at[strike, PLANES, own], S.at[strike, 0, own], 0, 1, 0)
    message("xy0", SE.at[strike, PLANES - 1], S.at[strike, 0, ghost_rows], 1, 1, 0)
    message("xa", XS.at[pl.ds(0, 10)], XR.at[pl.ds(0, 10)], 1, 0, 0)
    message("z0", PI.at[0, pl.ds(0, 64)], ZI.at[0, pl.ds(0, 64)], 0, 0, 1)
    message("xz0", PI.at[0, pl.ds(64, 8)], ZI.at[0, pl.ds(64, 8)], 1, 0, 1)
    loads["v"].wait()
    for i in range(6):
        loads[i].wait()
    message("xc", XS.at[pl.ds(10, 5)], XR.at[pl.ds(10, 5)], 1, 0, 0)
    message("yc", C.at[strike_c, PLANES, own], C.at[strike_c, 0, own], 0, 1, 0)
    message("xyc", CE.at[strike_c, PLANES - 1], C.at[strike_c, 0, ghost_rows], 1, 1, 0)
    accs = pack(C, C13, 1, PI.at[1], 16)
    message("zc", PI.at[1, pl.ds(0, 64)], ZI.at[1, pl.ds(0, 64)], 0, 0, 1)
    PI[1, pl.ds(64, 8)] = jnp.where(is_minus, pltpu.roll(accs[7], 64, 1), accs[0])
    message("xzc", PI.at[1, pl.ds(64, 8)], ZI.at[1, pl.ds(64, 8)], 1, 0, 1)

    for name in ("pre", "mask", "ids", "inv", "slip", "reg_a", "reg_n"):
        loads[name].wait()
    number = ids[...]
    picked_a = jnp.zeros((8, 128), f32)
    picked_n = jnp.zeros((8, 128), f32)
    for i in range(8):
        picked_a = jnp.where(number == i, reg_a[i], picked_a)
        picked_n = jnp.where(number == i, reg_n[i], picked_n)
    strength[...] = picked_a * picked_n

    def columns(src, dst):
        for t in range(TILES):
            tile = src[pl.ds(8 * (t // 2), 8)]
            for c in range(3):
                shift = (-16 * c - 64 * (t % 2)) % 128
                dst[c, rows(t)] = pltpu.roll(tile, shift, 1) if shift else tile

    arrived("z0")
    arrived("xz0")

    @pl.when(dn_z)
    def _():
        columns(ZI.at[0], SG)

    own_tiles = range(TILES - 1)
    all_tiles = range(TILES)

    def planes(first, last, body):
        def step(y, carry):
            body(y)
            return carry

        lax.fori_loop(first, last, step, 0)

    planes(1, PLANES, lambda y: trial(y, own_tiles))

    def columns_early(k):
        pack(V, 0, 0, PK.at[k, 0], TILES, early)
        message(("zb1", k), PK.at[k, 0], ZN.at[k, 0], 0, 0, -1)
        if k < STEPS - 1:
            message(("zf1", k), PK.at[k, 0], ZM.at[k, 0], 0, 0, 1)

    columns_early(0)
    arrived("xa")
    for n in range(10):
        spread(n)
    arrived("xy0")
    for y in range(PLANES):
        FB[6, pl.ds(y, 1)] = C[BUO, y + 1, pl.ds(own_f, 1)]
        FB[7, pl.ds(y, 1)] = C[BUO, y + 1, pl.ds(other_f, 1)]
    for y in range(PLANES):
        trial(y, [TILES - 1])
    arrived("y0")
    planes(0, 1, lambda y: trial(y, own_tiles))

    for k in range(STEPS):
        last = k == STEPS - 1
        fault()
        if not last:
            corners(k)
            message(("d1", k), CK.at[k], ZD1.at[k], 0, -1, 1)
            message(("d2", k), CK.at[k], ZD2.at[k], 0, 1, -1)
        message(("yb", k), V.at[:, 0], VN.at[k], 0, -1, 0)
        if not last:
            message(("yf", k), V.at[:, PLANES - 1], VP.at[k], 0, 1, 0)
        else:
            slip_out[...] = slip[...]

            def copy_plane(y):
                for c in range(3):
                    vel_out[c, y] = V[c, y, own]

            planes(0, PLANES, copy_plane)
        pack(V, 0, 0, PK.at[k, 1], TILES, lambda y, t: not early(y, t))
        message(("zb", k), PK.at[k, 1], ZN.at[k, 1], 0, 0, -1)
        if not last:
            message(("zf", k), PK.at[k, 1], ZM.at[k, 1], 0, 0, 1)
        if k == 0:
            arrived("zc")
            arrived("xzc")

            @pl.when(dn_z)
            def _():
                columns(ZI.at[1], CG)

            arrived("xc")
            for n in range(10, 15):
                spread(n)
            gone("y0")
        arrived(("zb1", k))
        unpack(ZN.at[k, 0], UN)
        planes(1, PLANES - 1, functools.partial(stress_own, k, INNER))
        arrived(("zb", k))
        merge(ZN.at[k], UN)
        for y in range(1, PLANES - 1):
            stress_own(k, FAULT, y)
        stress_own(k, all_tiles, 0)
        if last:
            arrived(("yb", k))
            stress_last(k)
            break
        arrived(("zf1", k))
        arrived(("zf", k))

        @pl.when(dn_z)
        def _():
            merge(ZM.at[k], UM)
            merge(PK.at[k], UO)
            column_ghost()

        planes(1, PLANES - 1, lambda y: trial(y, all_tiles))
        columns_early(k + 1)
        if k == 0:
            arrived("yc")
            arrived("xyc")
        arrived(("d1", k))
        arrived(("d2", k))
        gone(("yb", k))
        gone(("yf", k))
        arrived(("yf", k))
        arrived(("yb", k))
        column_corner(k)
        stress_ghost(k)
        stress_last(k)
        trial(0, all_tiles)
        trial(PLANES - 1, all_tiles)

    for name in list(sent):
        gone(name)


def writer(vel_in, str_in, slip_in, vel_out, str_out, slip_out, sem):
    pairs = [(slip_in, slip_out)]
    pairs += [(str_in.at[i], str_out.at[i]) for i in range(6)]
    pairs += [(vel_in.at[i], vel_out.at[i]) for i in range(3)]
    copies = [pltpu.make_async_copy(src, dst, sem.at[i]) for i, (src, dst) in enumerate(pairs)]
    for copy in copies:
        copy.start()
    for copy in copies:
        copy.wait()


def local(
    velocity, stress, buoyancy, stiff_xx, stiff_xz, stiff_zz, shear_vert, shear_horiz,
    prestress, fault_mask, region_ids, inverse_rate, slip_prev, region_a, region_normal,
):
    f32 = jnp.float32
    hbm = pl.BlockSpec(memory_space=pltpu.HBM)
    vmem = pl.BlockSpec(memory_space=pltpu.VMEM)
    tile = pltpu.VMEM((8, 128), f32)
    plane = (EXT, 128)
    packed = (72, 128)
    corner = (16, 128)
    large = [
        pltpu.with_memory_space_constraint(x, pltpu.HBM)
        for x in (
            velocity, stress, buoyancy, stiff_xx, stiff_xz, stiff_zz, shear_vert, shear_horiz,
            prestress, fault_mask, region_ids, inverse_rate, slip_prev, region_a, region_normal,
        )
    ]
    results = pl.pallas_call(
        kernel,
        out_shape=(
            jax.ShapeDtypeStruct(velocity.shape, f32),
            jax.ShapeDtypeStruct(stress.shape, f32),
            jax.ShapeDtypeStruct(slip_prev.shape, f32),
        ),
        in_specs=[hbm] * 15,
        out_specs=(vmem, vmem, vmem),
        scratch_shapes=[
            pltpu.VMEM((6, PLANES + 1) + plane, f32),
            pltpu.VMEM((3, PLANES) + plane, f32),
            pltpu.VMEM((6, PLANES + 1) + plane, f32),
            pltpu.VMEM((STEPS, 3) + plane, f32),
            pltpu.VMEM((STEPS - 1, 3) + plane, f32),
            pltpu.VMEM((STEPS, 2) + packed, f32),
            pltpu.VMEM((STEPS, 2) + packed, f32),
            pltpu.VMEM((STEPS - 1, 2) + packed, f32),
            pltpu.VMEM((5,) + plane, f32),
            pltpu.VMEM((STEPS - 1,) + corner, f32),
            pltpu.VMEM((STEPS - 1,) + corner, f32),
            pltpu.VMEM((STEPS - 1,) + corner, f32),
            pltpu.VMEM((2,) + packed, f32),
            pltpu.VMEM((2,) + packed, f32),
            pltpu.VMEM(plane, f32),
            pltpu.VMEM(plane, f32),
            pltpu.VMEM(plane, f32),
            pltpu.VMEM((3,) + plane, f32),
            pltpu.VMEM((3,) + plane, f32),
            pltpu.VMEM((8, 8, 128), f32),
            pltpu.VMEM((6, PLANES, 8, 128), f32),
            pltpu.VMEM((3, PLANES, 8, 128), f32),
            pltpu.VMEM((6, PLANES, 8, 128), f32),
            pltpu.VMEM((15, PLANES // 2, 8, 128), f32),
            pltpu.VMEM((15, PLANES // 2, 8, 128), f32),
            pltpu.VMEM((2, 8, 128), f32),
            pltpu.VMEM((8, 128), jnp.int32),
            pltpu.VMEM((8, 128), jnp.int32),
            tile,
            tile,
            tile,
            pltpu.SMEM((8,), f32),
            pltpu.SMEM((8,), f32),
            pltpu.SemaphoreType.DMA((40,)),
            pltpu.SemaphoreType.DMA((40,)),
            pltpu.SemaphoreType.DMA((40,)),
        ],
        compiler_params=pltpu.CompilerParams(
            collective_id=0, has_side_effects=True, vmem_limit_bytes=40 * 1024 * 1024
        ),
        name="rupture",
    )(*large)
    return pl.pallas_call(
        writer,
        out_shape=tuple(jax.ShapeDtypeStruct(x.shape, f32) for x in results),
        in_specs=[vmem] * 3,
        out_specs=(hbm, hbm, hbm),
        scratch_shapes=[pltpu.SemaphoreType.DMA((16,))],
        compiler_params=pltpu.CompilerParams(vmem_limit_bytes=1024 * 1024),
        name="writer",
    )(*results)


def solution(mesh):
    cell, fault_tile = P("gy", "gx", "gz"), P("gy", "gz")
    field = P(None, "gy", "gx", "gz")
    in_specs = (field, field) + (cell,) * 6 + (P(None, "gy", "gz"),) + (fault_tile,) * 4 + (P(), P())
    out_specs = (field, field, fault_tile)
    return jax.shard_map(local, mesh=mesh, in_specs=in_specs, out_specs=out_specs, check_vma=False)
```

```python
import functools

import jax
import jax.numpy as jnp
from jax import lax
from jax.experimental import pallas as pl
from jax.experimental.pallas import tpu as pltpu
from jax.sharding import PartitionSpec as P

STEPS = 3
NEWTON = 3
DT = 0.2
MESH = pl.DeviceIdType.MESH

S_ORDER = (0, 2, 4, 3, 1, 5)
XX, ZZ, XZ, YZ, YY, XY = range(6)
BUO, C11, C66, C13, C44, C33 = range(6)

PLANES = 8
ROWS = 128
TILES = 17
EXT = 8 * TILES

LOW, HIGH = 3, 13


def part_tiles(k, part):
    if part == 0:
        return [*range(LOW - k), *range(HIGH + k, TILES)]
    return [*range(LOW - k, HIGH + k)]


def part_rows(k, part):
    if part == 0:
        return [(0, 8 * (LOW - k)), (8 * (HIGH + k), EXT)]
    return [(8 * (LOW - k), 8 * (HIGH + k))]


def ghost_tiles(k, part):
    if part == 0:
        return [*range(LOW - k - 1), *range(HIGH + k, TILES)]
    return [*range(LOW - k - 1, HIGH + k)]


def kernel(
    vel_hbm, str_hbm, buo_hbm, c11_hbm, c13_hbm, c33_hbm, c44_hbm, c66_hbm,
    pre_hbm, mask_hbm, ids_hbm, inv_hbm, slip_hbm, reg_a_hbm, reg_n_hbm,
    vel_out, str_out, slip_out,
    S, V, C, VN, VP, PK, ZN, ZM, GP, CK, ZD1, ZD2, PI, ZI, UN, UM, UO, SG, CG,
    FB, SE, VE, CE, XS, XR, pre, mask, ids, inv, slip, strength, reg_a, reg_n,
    lsem, ssem, rsem,
):
    f32 = jnp.float32
    ngy, ngz = lax.axis_size("gy"), lax.axis_size("gz")
    gx, gy, gz = lax.axis_index("gx"), lax.axis_index("gy"), lax.axis_index("gz")
    is_minus = gx == 0
    lane = lax.broadcasted_iota(jnp.int32, (8, 128), 1)
    sub = lax.broadcasted_iota(jnp.int32, (8, 128), 0)
    edge = (1 - gx) * (ROWS - 8)
    own_f = (1 - gx) * (ROWS - 1)
    other_f = ROWS + gx * 7

    up_y, dn_y, up_z, dn_z = gy < ngy - 1, gy > 0, gz < ngz - 1, gz > 0

    def at(dx, dy, dz):
        return (
            gx if dx == 0 else 1 - gx,
            jnp.clip(gy + dy, 0, ngy - 1),
            jnp.clip(gz + dz, 0, ngz - 1),
        )

    def exists(dy, dz):
        ok = gy >= 0
        if dy:
            ok = jnp.logical_and(ok, up_y if dy > 0 else dn_y)
        if dz:
            ok = jnp.logical_and(ok, up_z if dz > 0 else dn_z)
        return ok

    barrier = pltpu.get_barrier_semaphore()
    around = [
        (0, 1, 0), (0, -1, 0), (0, 0, 1), (0, 0, -1), (0, -1, 1), (0, 1, -1),
        (1, 0, 0), (1, 1, 0), (1, -1, 0), (1, 0, 1), (1, 0, -1),
    ]
    count = jnp.int32(0)
    for dx, dy, dz in around:
        ok = exists(dy, dz)
        count = count + ok.astype(jnp.int32)

        @pl.when(ok)
        def _():
            pl.semaphore_signal(barrier, inc=1, device_id=at(dx, dy, dz), device_id_type=MESH)

    loads = {}

    def load(name, src, dst):
        copy = pltpu.make_async_copy(src, dst, lsem.at[len(loads)])
        copy.start()
        loads[name] = copy

    own = pl.ds(0, ROWS)
    edge_rows = pl.ds(pl.multiple_of(edge, 8), 8)
    for i in range(6):
        load(("se", i), str_hbm.at[S_ORDER[i], :, edge_rows], SE.at[i])
    load("ve", vel_hbm.at[:, :, edge_rows], VE)
    coefficients = ((BUO, buo_hbm), (C11, c11_hbm), (C66, c66_hbm), (C13, c13_hbm), (C44, c44_hbm), (C33, c33_hbm))
    for i, ref in coefficients:
        load(("ce", i), ref.at[:, edge_rows], CE.at[i])
    for i in (YZ, YY, XY):
        load(("s7", i), str_hbm.at[S_ORDER[i], PLANES - 1], S.at[i, PLANES, own])
    for i in (ZZ, XZ):
        load(("s", i), str_hbm.at[S_ORDER[i]], S.at[i, pl.ds(1, PLANES), own])
    for i in (YZ, YY, XY):
        load(("s", i), str_hbm.at[S_ORDER[i], pl.ds(0, PLANES - 1)], S.at[i, pl.ds(1, PLANES - 1), own])
    load(("s", XX), str_hbm.at[S_ORDER[XX]], S.at[XX, pl.ds(1, PLANES), own])
    load("v", vel_hbm, V.at[:, :, own])
    for i, ref in coefficients:
        load(i, ref, C.at[i, pl.ds(1, PLANES), own])
    load("pre", pre_hbm, pre)
    load("mask", mask_hbm, mask)
    load("ids", ids_hbm, ids)
    load("inv", inv_hbm, inv)
    load("slip", slip_hbm, slip)
    load("reg_a", reg_a_hbm, reg_a)
    load("reg_n", reg_n_hbm, reg_n)

    sent = {}

    def message(name, src, dst, dx, dy, dz):
        i = len(sent)
        copy = pltpu.make_async_remote_copy(
            src_ref=src, dst_ref=dst, send_sem=ssem.at[i], recv_sem=rsem.at[i],
            device_id=at(dx, dy, dz), device_id_type=MESH,
        )
        sent[name] = [copy, exists(dy, dz), exists(-dy, -dz), True]

        @pl.when(exists(dy, dz))
        def _():
            copy.start()

    def arrived(name):
        copy, _, source, _ = sent[name]

        @pl.when(source)
        def _():
            copy.wait_recv()

    def gone(name):
        copy, target, _, pending = sent[name]
        if pending:
            sent[name][3] = False

            @pl.when(target)
            def _():
                copy.wait_send()

    def rows(t):
        return pl.ds(8 * t, 8)

    def below(ref, lead, t):
        if t in (0, TILES - 1):
            return jnp.where(sub == 0, 0.0, pltpu.roll(ref[lead + (rows(t),)], 1, 0))
        return ref[lead + (pl.ds(8 * t - 1, 8),)]

    def above(ref, lead, t):
        if t in (TILES - 2, TILES - 1):
            return jnp.where(sub == 7, 0.0, pltpu.roll(ref[lead + (rows(t),)], 7, 0))
        return ref[lead + (pl.ds(8 * t + 1, 8),)]

    def pack(ref, lead, plane0, out, tiles):
        groups = (len(tiles) + 1) // 2

        def body(c, accs):
            accs = list(accs)
            for y in range(PLANES):
                for j, t in enumerate(tiles):
                    base = 64 * (j % 2) + 16 * c + 2 * y
                    moved = pltpu.roll(ref[lead + c, plane0 + y, rows(t)], base + 1, 1)
                    hit = jnp.logical_or(lane == base, lane == base + 1)
                    accs[j // 2] = jnp.where(hit, moved, accs[j // 2])
            return tuple(accs)

        accs = lax.fori_loop(0, 3, body, tuple(jnp.zeros((8, 128), f32) for _ in range(groups)))
        for g in range(groups):
            out[pl.ds(8 * g, 8)] = accs[g]
        return accs

    def unpack(src, dst, tiles):
        for j, t in enumerate(tiles):
            tile = src[pl.ds(8 * (j // 2), 8)]
            dst[rows(t)] = tile if j % 2 == 0 else pltpu.roll(tile, 64, 1)

    def corners(k, part):
        acc = jnp.zeros((8, 128), f32)
        for j, t in enumerate(part_tiles(k, part)):
            for c in range(3):
                base = 8 * j + 2 * c
                both = jnp.where(lane == 127, V[c, 0, rows(t)], V[c, PLANES - 1, rows(t)])
                hit = jnp.logical_or(lane == base, lane == base + 1)
                acc = jnp.where(hit, pltpu.roll(both, base + 1, 1), acc)
        CK[k, part] = acc

    def corner_of(ref, k, t, c, by):
        part = 0 if t in part_tiles(k, 0) else 1
        j = part_tiles(k, part).index(t)
        return pltpu.roll(ref[k, part], (by - 8 * j - 2 * c) % 128, 1)

    def trial(y, tiles):
        back = (128 - 2 * y) % 128 if isinstance(y, int) else lax.rem(128 - 2 * y, 128)

        def lower_dip(value, i, t):
            halo = SG[i, rows(t)]
            if not isinstance(back, int) or back:
                halo = pltpu.roll(halo, back, 1)
            return value - jnp.where(lane == 0, halo, pltpu.roll(value, 1, 1))

        for t in tiles:
            r = rows(t)
            sxx, szz, sxz, syz, syy, sxy = (S[i, y + 1, r] for i in range(6))
            scale = DT * C[BUO, y + 1, r]
            vx = V[0, y, r] + scale * (
                (sxx - below(S, (XX, y + 1), t)) + (sxy - S[XY, y, r]) + lower_dip(sxz, 1, t)
            )
            vy = V[1, y, r] + scale * (
                (sxy - below(S, (XY, y + 1), t)) + (syy - S[YY, y, r]) + lower_dip(syz, 2, t)
            )
            vz = V[2, y, r] + scale * (
                (sxz - below(S, (XZ, y + 1), t)) + (syz - S[YZ, y, r]) + lower_dip(szz, 0, t)
            )
            V[0, y, r] = vx
            V[1, y, r] = vy
            V[2, y, r] = vz

    def stress(p, here, here_lead, over, over_lead, halo, ghost=False, last=False, tiles=range(TILES)):
        def put(i, value):
            if ghost:
                S[i, p, r] = jnp.where(dn_y, value, S[i, p, r])
            elif last:
                str_out[S_ORDER[i], p - 1, r] = value
            else:
                S[i, p, r] = value

        for t in tiles:
            if last and t == TILES - 1:
                continue
            r = rows(t)

            def upper_dip(value, c):
                return jnp.where(lane == 127, halo(c, t), pltpu.roll(value, 127, 1)) - value

            vx, vy, vz = (here[here_lead(c) + (r,)] for c in range(3))
            ox, oy, oz = (over[over_lead(c) + (r,)] for c in range(3))
            exx = above(here, here_lead(0), t) - vx
            eyy = oy - vy
            ezz = upper_dip(vz, 2)
            c11, c66, c13, c44 = (C[i, p, r] for i in (C11, C66, C13, C44))
            lame = c11 - 2.0 * c66
            put(YY, S[YY, p, r] + DT * (lame * exx + c11 * eyy + c13 * ezz))
            put(YZ, S[YZ, p, r] + DT * c44 * (upper_dip(vy, 1) + (oz - vz)))
            put(XY, S[XY, p, r] + DT * c66 * ((ox - vx) + (above(here, here_lead(1), t) - vy)))
            if not ghost:
                put(XX, S[XX, p, r] + DT * (c11 * exx + lame * eyy + c13 * ezz))
                put(ZZ, S[ZZ, p, r] + DT * (c13 * (exx + eyy) + C[C33, p, r] * ezz))
                put(XZ, S[XZ, p, r] + DT * c44 * (
                    upper_dip(vx, 0) + (above(here, here_lead(2), t) - vz)
                ))

    def next_dip(y):
        return lambda c, t: pltpu.roll(UN[rows(t)], 126 - 16 * c - 2 * y, 1)

    def stress_own(k, tiles, y):
        stress(
            y + 1, V, lambda c: (c, y), V, lambda c: (c, y + 1), next_dip(y),
            last=k == STEPS - 1, tiles=tiles,
        )

    def stress_last(k, tiles):
        stress(PLANES, V, lambda c: (c, PLANES - 1), VN, lambda c: (k, c), next_dip(PLANES - 1), last=k == STEPS - 1, tiles=tiles)

    def stress_ghost(k, tiles):
        stress(0, VP, lambda c: (k, c), V, lambda c: (c, 0), lambda c, t: corner_of(ZD2, k, t, c, 126), ghost=True, tiles=tiles)

    def column_ghost(tiles):
        for t in tiles:
            r = rows(t)

            def shifted(ref, by):
                return pltpu.roll(ref[r], by % 128, 1)

            def upper_rows(c):
                if t in (TILES - 2, TILES - 1):
                    return pltpu.roll(
                        jnp.where(sub == 7, 0.0, pltpu.roll(UM[r], 7, 0)), (-16 * c) % 128, 1
                    )
                return pltpu.roll(UM[pl.ds(8 * t + 1, 8)], (-16 * c) % 128, 1)

            vx, vy, vz = UM[r], shifted(UM, -16), shifted(UM, -32)
            ox, oy, oz = shifted(UO, -1), shifted(UO, -17), shifted(UO, -33)
            exx = upper_rows(0) - vx
            eyy = pltpu.roll(vy, 126, 1) - vy
            ezz = oz - vz
            c13, c44, c33 = CG[0, r], CG[1, r], CG[2, r]
            zz = SG[0, r] + DT * (c13 * (exx + eyy) + c33 * ezz)
            yz = SG[2, r] + DT * c44 * ((oy - vy) + (pltpu.roll(vz, 126, 1) - vz))
            SG[0, r] = jnp.where(lane == 14, SG[0, r], zz)
            SG[1, r] = SG[1, r] + DT * c44 * ((ox - vx) + (upper_rows(2) - vz))
            SG[2, r] = jnp.where(lane == 14, SG[2, r], yz)
            for i, value in enumerate((exx, vy, ezz, oy - vy, vz)):
                GP[i, r] = value

    def column_corner(k, tiles):
        here = jnp.logical_and(lane == 14, dn_z)
        for t in tiles:
            r = rows(t)
            exx, vy, ezz, oy_vy, vz = (GP[i, r] for i in range(5))
            eyy = corner_of(ZD1, k, t, 1, 14) - vy
            c13, c44, c33 = CG[0, r], CG[1, r], CG[2, r]
            zz = SG[0, r] + DT * (c13 * (exx + eyy) + c33 * ezz)
            yz = SG[2, r] + DT * c44 * (oy_vy + (corner_of(ZD1, k, t, 2, 14) - vz))
            SG[0, r] = jnp.where(here, zz, SG[0, r])
            SG[2, r] = jnp.where(here, yz, SG[2, r])

    def fault():
        for c in range(3):
            for y in range(PLANES):
                FB[c, pl.ds(y, 1)] = V[c, y, pl.ds(own_f, 1)]
                FB[3 + c, pl.ds(y, 1)] = V[c, y, pl.ds(other_f, 1)]
        own_v, other_v = [FB[c] for c in range(3)], [FB[3 + c] for c in range(3)]
        own_b, other_b = FB[6], FB[7]
        minus_b = jnp.where(is_minus, own_b, other_b)
        plus_b = jnp.where(is_minus, other_b, own_b)
        minus_v = [jnp.where(is_minus, a, b) for a, b in zip(own_v, other_v)]
        plus_v = [jnp.where(is_minus, b, a) for a, b in zip(own_v, other_v)]
        impedance = 1.0 / (DT * (minus_b + plus_b))
        jump = [b - a for a, b in zip(minus_v, plus_v)]
        locked_y = pre[0] + impedance * jump[1]
        locked_z = pre[1] + impedance * jump[2]
        magnitude = jnp.sqrt(locked_y * locked_y + locked_z * locked_z + 1.0)
        hold = strength[...]
        rate = inv[...]
        value = slip[...]
        for _ in range(NEWTON):
            scaled = rate * value
            size = jnp.abs(scaled)
            root = jnp.sqrt(size * size + 1.0)
            log = jnp.log(size + root)
            residual = magnitude - impedance * value - hold * jnp.where(scaled < 0.0, -log, log)
            tangent = -impedance - hold * rate / root
            value = value - residual / tangent
        value = value * mask[...].astype(f32)
        slip[...] = value
        retained = 1.0 - impedance * value / magnitude
        traction = [impedance * jump[0], retained * locked_y - pre[0], retained * locked_z - pre[1]]
        for c in range(3):
            minus_new = minus_v[c] + DT * minus_b * traction[c]
            plus_new = plus_v[c] - DT * plus_b * traction[c]
            FB[c] = jnp.where(is_minus, minus_new, plus_new)
            FB[3 + c] = jnp.where(is_minus, plus_new, minus_new)
        for c in range(3):
            for y in range(PLANES):
                V[c, y, pl.ds(own_f, 1)] = FB[c, pl.ds(y, 1)]
                V[c, y, pl.ds(other_f, 1)] = FB[3 + c, pl.ds(y, 1)]

    @pl.when(jnp.logical_not(up_y))
    def _():
        VN[...] = jnp.zeros(VN.shape, f32)
        ZD1[...] = jnp.zeros(ZD1.shape, f32)

    @pl.when(jnp.logical_not(dn_y))
    def _():
        S[pl.ds(YZ, 3), 0] = jnp.zeros((3, EXT, 128), f32)

    @pl.when(jnp.logical_not(up_z))
    def _():
        ZN[...] = jnp.zeros(ZN.shape, f32)
        ZD2[...] = jnp.zeros(ZD2.shape, f32)

    @pl.when(jnp.logical_not(dn_z))
    def _():
        SG[...] = jnp.zeros(SG.shape, f32)

    ghost_rows = pl.ds(ROWS, 8)
    strike = pl.ds(YZ, 3)
    strike_c = pl.ds(C11, 4)
    for i in (YZ, YY, XY):
        loads["s7", i].wait()
    for i in range(6):
        loads["se", i].wait()
    loads["ve"].wait()
    for i in range(6):
        loads["ce", i].wait()
    fields = [(SE, S, i, 1) for i in range(6)] + [(VE, V, i, 0) for i in range(3)]
    fields += [(CE, C, i, 1) for i in range(6)]
    for n, (src, _, i, _) in enumerate(fields):
        for q in range(PLANES // 2):
            first, second = src[i, 2 * q], src[i, 2 * q + 1]
            low = jnp.where(is_minus, pltpu.roll(first, 4, 0), first)
            high = jnp.where(is_minus, second, pltpu.roll(second, 4, 0))
            XS[n, q] = jnp.where(sub < 4, low, high)

    def spread(n):
        _, dst, i, base = fields[n]
        for q in range(PLANES // 2):
            value = XR[n, q]
            moved = pltpu.roll(value, 4, 0)
            dst[i, base + 2 * q, ghost_rows] = jnp.where(is_minus, value, moved)
            dst[i, base + 2 * q + 1, ghost_rows] = jnp.where(is_minus, moved, value)

    for i in (ZZ, XZ, YZ, YY, XY, XX):
        loads["s", i].wait()
    accs = pack(S, ZZ, 1, PI.at[0], range(16))
    PI[0, pl.ds(64, 8)] = jnp.where(is_minus, pltpu.roll(accs[7], 64, 1), accs[0])
    pl.semaphore_wait(barrier, count)
    first_rows = [(0, 8 * LOW), (8 * HIGH, ROWS), (8 * LOW, 8 * HIGH)]
    for i, (top, end) in enumerate(first_rows[:2]):
        some = pl.ds(top, end - top)
        message(("y0", i), S.at[strike, PLANES, some], S.at[strike, 0, some], 0, 1, 0)
    message("xy0", SE.at[strike, PLANES - 1], S.at[strike, 0, ghost_rows], 1, 1, 0)
    mid = pl.ds(8 * LOW, 8 * (HIGH - LOW))
    message(("y0", 2), S.at[strike, PLANES, mid], S.at[strike, 0, mid], 0, 1, 0)
    message("xa", XS.at[pl.ds(0, 10)], XR.at[pl.ds(0, 10)], 1, 0, 0)
    message("z0", PI.at[0, pl.ds(0, 64)], ZI.at[0, pl.ds(0, 64)], 0, 0, 1)
    message("xz0", PI.at[0, pl.ds(64, 8)], ZI.at[0, pl.ds(64, 8)], 1, 0, 1)
    loads["v"].wait()
    for i in range(6):
        loads[i].wait()
    message("xc", XS.at[pl.ds(10, 5)], XR.at[pl.ds(10, 5)], 1, 0, 0)
    message("yc", C.at[strike_c, PLANES, own], C.at[strike_c, 0, own], 0, 1, 0)
    message("xyc", CE.at[strike_c, PLANES - 1], C.at[strike_c, 0, ghost_rows], 1, 1, 0)
    accs = pack(C, C13, 1, PI.at[1], range(16))
    message("zc", PI.at[1, pl.ds(0, 64)], ZI.at[1, pl.ds(0, 64)], 0, 0, 1)
    PI[1, pl.ds(64, 8)] = jnp.where(is_minus, pltpu.roll(accs[7], 64, 1), accs[0])
    message("xzc", PI.at[1, pl.ds(64, 8)], ZI.at[1, pl.ds(64, 8)], 1, 0, 1)

    for name in ("pre", "mask", "ids", "inv", "slip", "reg_a", "reg_n"):
        loads[name].wait()
    number = ids[...]
    picked_a = jnp.zeros((8, 128), f32)
    picked_n = jnp.zeros((8, 128), f32)
    for i in range(8):
        picked_a = jnp.where(number == i, reg_a[i], picked_a)
        picked_n = jnp.where(number == i, reg_n[i], picked_n)
    strength[...] = picked_a * picked_n

    def columns(src, dst):
        for t in range(TILES):
            tile = src[pl.ds(8 * (t // 2), 8)]
            for c in range(3):
                shift = (-16 * c - 64 * (t % 2)) % 128
                dst[c, rows(t)] = pltpu.roll(tile, shift, 1) if shift else tile

    arrived("z0")
    arrived("xz0")

    @pl.when(dn_z)
    def _():
        columns(ZI.at[0], SG)

    own_tiles = range(TILES - 1)
    all_tiles = range(TILES)

    def planes(first, last, body):
        def step(y, carry):
            body(y)
            return carry

        lax.fori_loop(first, last, step, 0)

    planes(1, PLANES, lambda y: trial(y, own_tiles))

    def send_strike(k, part):
        if k < STEPS - 1:
            corners(k, part)
            message(("d1", k, part), CK.at[k, part], ZD1.at[k, part], 0, -1, 1)
            message(("d2", k, part), CK.at[k, part], ZD2.at[k, part], 0, 1, -1)
        for i, (top, end) in enumerate(part_rows(k, part)):
            some = pl.ds(top, end - top)
            message(("yb", k, part, i), V.at[:, 0, some], VN.at[k, :, some], 0, -1, 0)
            if k < STEPS - 1:
                message(("yf", k, part, i), V.at[:, PLANES - 1, some], VP.at[k, :, some], 0, 1, 0)

    def send_dip(k, part):
        tiles = part_tiles(k, part)
        size = pl.ds(0, 8 * ((len(tiles) + 1) // 2))
        pack(V, 0, 0, PK.at[k, part], tiles)
        message(("zb", k, part), PK.at[k, part, size], ZN.at[k, part, size], 0, 0, -1)
        if k < STEPS - 1:
            message(("zf", k, part), PK.at[k, part, size], ZM.at[k, part, size], 0, 0, 1)

    def interior(k, part):
        tiles = part_tiles(k, part)
        arrived(("zb", k, part))
        unpack(ZN.at[k, part], UN, tiles)
        if part == 0:
            for y in range(PLANES - 1):
                stress_own(k, tiles, y)
        else:
            stress_own(k, tiles, 0)

            def two(i):
                stress_own(k, tiles, 2 * i + 1)
                stress_own(k, tiles, 2 * i + 2)

            planes(0, PLANES // 2 - 1, two)
        if k == STEPS - 1:
            return
        arrived(("zf", k, part))

        @pl.when(dn_z)
        def _():
            unpack(ZM.at[k, part], UM, tiles)
            unpack(PK.at[k, part], UO, tiles)
            column_ghost(ghost_tiles(k, part))

        after = part_tiles(k + 1, part)
        if part == 0:
            for y in range(1, PLANES - 1):
                trial(y, after)
        else:

            def two_trials(i):
                trial(2 * i + 1, after)
                trial(2 * i + 2, after)

            planes(0, PLANES // 2 - 1, two_trials)

    def boundary(k, part):
        if k == 0 and part == 0:
            arrived("yc")
            arrived("xyc")
        for name in ("d1", "d2"):
            arrived((name, k, part))
        for i in range(len(part_rows(k, part))):
            for name in ("yf", "yb"):
                gone((name, k, part, i))
                arrived((name, k, part, i))
        column_corner(k, ghost_tiles(k, part))
        stress_ghost(k, ghost_tiles(k, part))
        stress_last(k, part_tiles(k, part))
        after = part_tiles(k + 1, part)
        trial(0, after)
        trial(PLANES - 1, after)

    arrived("xa")
    for n in range(10):
        spread(n)
    for y in range(PLANES):
        FB[6, pl.ds(y, 1)] = C[BUO, y + 1, pl.ds(own_f, 1)]
        FB[7, pl.ds(y, 1)] = C[BUO, y + 1, pl.ds(other_f, 1)]
    for y in range(1, PLANES):
        trial(y, [TILES - 1])
    arrived("xy0")
    arrived(("y0", 0))
    arrived(("y0", 1))
    trial(0, part_tiles(0, 0))
    fault()
    send_strike(0, 0)
    send_dip(0, 0)
    arrived(("y0", 2))
    trial(0, part_tiles(0, 1))
    send_strike(0, 1)
    send_dip(0, 1)

    arrived("zc")
    arrived("xzc")

    @pl.when(dn_z)
    def _():
        columns(ZI.at[1], CG)

    arrived("xc")
    for n in range(10, 15):
        spread(n)
    for i in range(3):
        gone(("y0", i))

    for k in range(STEPS - 1):
        interior(k, 0)
        boundary(k, 0)
        fault()
        send_strike(k + 1, 0)
        send_dip(k + 1, 0)
        interior(k, 1)
        boundary(k, 1)
        send_strike(k + 1, 1)
        send_dip(k + 1, 1)

    k = STEPS - 1
    slip_out[...] = slip[...]

    def copy_plane(y):
        for c in range(3):
            vel_out[c, y] = V[c, y, own]

    planes(0, PLANES, copy_plane)
    for part in range(2):
        interior(k, part)
    for part in range(2):
        for i in range(len(part_rows(k, part))):
            arrived(("yb", k, part, i))
        stress_last(k, part_tiles(k, part))

    for name in list(sent):
        gone(name)


def writer(vel_in, str_in, slip_in, vel_out, str_out, slip_out, sem):
    pairs = [(slip_in, slip_out)]
    pairs += [(str_in.at[i], str_out.at[i]) for i in range(6)]
    pairs += [(vel_in.at[i], vel_out.at[i]) for i in range(3)]
    copies = [pltpu.make_async_copy(src, dst, sem.at[i]) for i, (src, dst) in enumerate(pairs)]
    for copy in copies:
        copy.start()
    for copy in copies:
        copy.wait()


def local(
    velocity, stress, buoyancy, stiff_xx, stiff_xz, stiff_zz, shear_vert, shear_horiz,
    prestress, fault_mask, region_ids, inverse_rate, slip_prev, region_a, region_normal,
):
    f32 = jnp.float32
    hbm = pl.BlockSpec(memory_space=pltpu.HBM)
    vmem = pl.BlockSpec(memory_space=pltpu.VMEM)
    tile = pltpu.VMEM((8, 128), f32)
    plane = (EXT, 128)
    packed = (72, 128)
    half = (56, 128)
    corner = (2, 8, 128)
    large = [
        pltpu.with_memory_space_constraint(x, pltpu.HBM)
        for x in (
            velocity, stress, buoyancy, stiff_xx, stiff_xz, stiff_zz, shear_vert, shear_horiz,
            prestress, fault_mask, region_ids, inverse_rate, slip_prev, region_a, region_normal,
        )
    ]
    results = pl.pallas_call(
        kernel,
        out_shape=(
            jax.ShapeDtypeStruct(velocity.shape, f32),
            jax.ShapeDtypeStruct(stress.shape, f32),
            jax.ShapeDtypeStruct(slip_prev.shape, f32),
        ),
        in_specs=[hbm] * 15,
        out_specs=(vmem, vmem, vmem),
        scratch_shapes=[
            pltpu.VMEM((6, PLANES + 1) + plane, f32),
            pltpu.VMEM((3, PLANES) + plane, f32),
            pltpu.VMEM((6, PLANES + 1) + plane, f32),
            pltpu.VMEM((STEPS, 3) + plane, f32),
            pltpu.VMEM((STEPS - 1, 3) + plane, f32),
            pltpu.VMEM((STEPS, 2) + half, f32),
            pltpu.VMEM((STEPS, 2) + half, f32),
            pltpu.VMEM((STEPS - 1, 2) + half, f32),
            pltpu.VMEM((5,) + plane, f32),
            pltpu.VMEM((STEPS - 1,) + corner, f32),
            pltpu.VMEM((STEPS - 1,) + corner, f32),
            pltpu.VMEM((STEPS - 1,) + corner, f32),
            pltpu.VMEM((2,) + packed, f32),
            pltpu.VMEM((2,) + packed, f32),
            pltpu.VMEM(plane, f32),
            pltpu.VMEM(plane, f32),
            pltpu.VMEM(plane, f32),
            pltpu.VMEM((3,) + plane, f32),
            pltpu.VMEM((3,) + plane, f32),
            pltpu.VMEM((8, 8, 128), f32),
            pltpu.VMEM((6, PLANES, 8, 128), f32),
            pltpu.VMEM((3, PLANES, 8, 128), f32),
            pltpu.VMEM((6, PLANES, 8, 128), f32),
            pltpu.VMEM((15, PLANES // 2, 8, 128), f32),
            pltpu.VMEM((15, PLANES // 2, 8, 128), f32),
            pltpu.VMEM((2, 8, 128), f32),
            pltpu.VMEM((8, 128), jnp.int32),
            pltpu.VMEM((8, 128), jnp.int32),
            tile,
            tile,
            tile,
            pltpu.SMEM((8,), f32),
            pltpu.SMEM((8,), f32),
            pltpu.SemaphoreType.DMA((40,)),
            pltpu.SemaphoreType.DMA((64,)),
            pltpu.SemaphoreType.DMA((64,)),
        ],
        compiler_params=pltpu.CompilerParams(
            collective_id=0, has_side_effects=True, vmem_limit_bytes=40 * 1024 * 1024
        ),
        name="rupture",
    )(*large)
    return pl.pallas_call(
        writer,
        out_shape=tuple(jax.ShapeDtypeStruct(x.shape, f32) for x in results),
        in_specs=[vmem] * 3,
        out_specs=(hbm, hbm, hbm),
        scratch_shapes=[pltpu.SemaphoreType.DMA((16,))],
        compiler_params=pltpu.CompilerParams(vmem_limit_bytes=1024 * 1024),
        name="writer",
    )(*results)


def solution(mesh):
    cell, fault_tile = P("gy", "gx", "gz"), P("gy", "gz")
    field = P(None, "gy", "gx", "gz")
    in_specs = (field, field) + (cell,) * 6 + (P(None, "gy", "gz"),) + (fault_tile,) * 4 + (P(), P())
    out_specs = (field, field, fault_tile)
    return jax.shard_map(local, mesh=mesh, in_specs=in_specs, out_specs=out_specs, check_vma=False)
```

```python
import functools

import jax
import jax.numpy as jnp
from jax import lax
from jax.experimental import pallas as pl
from jax.experimental.pallas import tpu as pltpu
from jax.sharding import PartitionSpec as P

STEPS = 3
NEWTON = 3
DT = 0.2
MESH = pl.DeviceIdType.MESH

S_ORDER = (0, 2, 4, 3, 1, 5)
XX, ZZ, XZ, YZ, YY, XY = range(6)
BUO, C11, C66, C13, C44, C33 = range(6)

PLANES = 8
ROWS = 128
TILES = 17
EXT = 8 * TILES
GHOST = slice(ROWS, EXT)


def kernel(
    vel_hbm, str_hbm, buo_hbm, c11_hbm, c13_hbm, c33_hbm, c44_hbm, c66_hbm,
    pre_hbm, mask_hbm, ids_hbm, inv_hbm, slip_hbm, reg_a_hbm, reg_n_hbm,
    vel_out, str_out, slip_out,
    S, V, C, VN, VP, PK, ZN, ZM, GP, CK, ZD1, ZD2, PI, ZI, UN, UM, UO, SG, CG,
    FB, SE, VE, CE, XS, XR, pre, mask, ids, inv, slip, strength, reg_a, reg_n,
    lsem, ssem, rsem,
):
    f32 = jnp.float32
    ngy, ngz = lax.axis_size("gy"), lax.axis_size("gz")
    gx, gy, gz = lax.axis_index("gx"), lax.axis_index("gy"), lax.axis_index("gz")
    is_minus = gx == 0
    lane = lax.broadcasted_iota(jnp.int32, (8, 128), 1)
    sub = lax.broadcasted_iota(jnp.int32, (8, 128), 0)
    edge = (1 - gx) * (ROWS - 8)
    own_f = (1 - gx) * (ROWS - 1)
    other_f = ROWS + gx * 7

    up_y, dn_y, up_z, dn_z = gy < ngy - 1, gy > 0, gz < ngz - 1, gz > 0

    def at(dx, dy, dz):
        return (
            gx if dx == 0 else 1 - gx,
            jnp.clip(gy + dy, 0, ngy - 1),
            jnp.clip(gz + dz, 0, ngz - 1),
        )

    def exists(dy, dz):
        ok = gy >= 0
        if dy:
            ok = jnp.logical_and(ok, up_y if dy > 0 else dn_y)
        if dz:
            ok = jnp.logical_and(ok, up_z if dz > 0 else dn_z)
        return ok

    barrier = pltpu.get_barrier_semaphore()
    around = [
        (0, 1, 0), (0, -1, 0), (0, 0, 1), (0, 0, -1), (0, -1, 1), (0, 1, -1),
        (1, 0, 0), (1, 1, 0), (1, -1, 0), (1, 0, 1), (1, 0, -1),
    ]
    count = jnp.int32(0)
    for dx, dy, dz in around:
        ok = exists(dy, dz)
        count = count + ok.astype(jnp.int32)

        @pl.when(ok)
        def _():
            pl.semaphore_signal(barrier, inc=1, device_id=at(dx, dy, dz), device_id_type=MESH)

    loads = {}

    def load(name, src, dst):
        copy = pltpu.make_async_copy(src, dst, lsem.at[len(loads)])
        copy.start()
        loads[name] = copy

    own = pl.ds(0, ROWS)
    edge_rows = pl.ds(pl.multiple_of(edge, 8), 8)
    for i in range(6):
        load(("se", i), str_hbm.at[S_ORDER[i], :, edge_rows], SE.at[i])
    load("ve", vel_hbm.at[:, :, edge_rows], VE)
    coefficients = ((BUO, buo_hbm), (C11, c11_hbm), (C66, c66_hbm), (C13, c13_hbm), (C44, c44_hbm), (C33, c33_hbm))
    for i, ref in coefficients:
        load(("ce", i), ref.at[:, edge_rows], CE.at[i])
    for i in (YZ, YY, XY):
        load(("s7", i), str_hbm.at[S_ORDER[i], PLANES - 1], S.at[i, PLANES, own])
    for i in (ZZ, XZ):
        load(("s", i), str_hbm.at[S_ORDER[i]], S.at[i, pl.ds(1, PLANES), own])
    for i in (YZ, YY, XY):
        load(("s", i), str_hbm.at[S_ORDER[i], pl.ds(0, PLANES - 1)], S.at[i, pl.ds(1, PLANES - 1), own])
    load(("s", XX), str_hbm.at[S_ORDER[XX]], S.at[XX, pl.ds(1, PLANES), own])
    load("v", vel_hbm, V.at[:, :, own])
    for i, ref in coefficients:
        load(i, ref, C.at[i, pl.ds(1, PLANES), own])
    load("pre", pre_hbm, pre)
    load("mask", mask_hbm, mask)
    load("ids", ids_hbm, ids)
    load("inv", inv_hbm, inv)
    load("slip", slip_hbm, slip)
    load("reg_a", reg_a_hbm, reg_a)
    load("reg_n", reg_n_hbm, reg_n)

    sent = {}

    def message(name, src, dst, dx, dy, dz):
        i = len(sent)
        copy = pltpu.make_async_remote_copy(
            src_ref=src, dst_ref=dst, send_sem=ssem.at[i], recv_sem=rsem.at[i],
            device_id=at(dx, dy, dz), device_id_type=MESH,
        )
        sent[name] = [copy, exists(dy, dz), exists(-dy, -dz), True]

        @pl.when(exists(dy, dz))
        def _():
            copy.start()

    def arrived(name):
        copy, _, source, _ = sent[name]

        @pl.when(source)
        def _():
            copy.wait_recv()

    def gone(name):
        copy, target, _, pending = sent[name]
        if pending:
            sent[name][3] = False

            @pl.when(target)
            def _():
                copy.wait_send()

    def rows(t):
        return pl.ds(8 * t, 8)

    def below(ref, lead, t):
        if t in (0, TILES - 1):
            return jnp.where(sub == 0, 0.0, pltpu.roll(ref[lead + (rows(t),)], 1, 0))
        return ref[lead + (pl.ds(8 * t - 1, 8),)]

    def above(ref, lead, t):
        if t in (TILES - 2, TILES - 1):
            return jnp.where(sub == 7, 0.0, pltpu.roll(ref[lead + (rows(t),)], 7, 0))
        return ref[lead + (pl.ds(8 * t + 1, 8),)]

    def pack(ref, lead, plane0, out, tiles, pick=lambda y, t: True):
        groups = (tiles + 1) // 2

        def body(c, accs):
            accs = list(accs)
            for y in range(PLANES):
                for t in range(tiles):
                    if not pick(y, t):
                        continue
                    base = 64 * (t % 2) + 16 * c + 2 * y
                    moved = pltpu.roll(ref[lead + c, plane0 + y, rows(t)], base + 1, 1)
                    hit = jnp.logical_or(lane == base, lane == base + 1)
                    accs[t // 2] = jnp.where(hit, moved, accs[t // 2])
            return tuple(accs)

        accs = lax.fori_loop(0, 3, body, tuple(jnp.zeros((8, 128), f32) for _ in range(groups)))
        for g in range(groups):
            out[pl.ds(8 * g, 8)] = accs[g]
        return accs

    FAULT = (0, TILES - 2, TILES - 1)
    INNER = range(1, TILES - 2)

    def early(y, t):
        return 0 < y < PLANES - 1 and t in INNER

    def merge(src, dst):
        strike_index = lax.rem(lane, 16) // 2
        outer = jnp.logical_or(strike_index == 0, strike_index == PLANES - 1)
        for g in range((TILES + 1) // 2):
            late = outer
            if 2 * g in FAULT:
                late = jnp.logical_or(late, lane < 64)
            if 2 * g + 1 in FAULT:
                late = jnp.logical_or(late, lane >= 64)
            tile = jnp.where(late, src[1, pl.ds(8 * g, 8)], src[0, pl.ds(8 * g, 8)])
            dst[rows(2 * g)] = tile
            if 2 * g + 1 < TILES:
                dst[rows(2 * g + 1)] = pltpu.roll(tile, 64, 1)

    def unpack(src, dst):
        for t in range(TILES):
            tile = src[pl.ds(8 * (t // 2), 8)]
            dst[rows(t)] = tile if t % 2 == 0 else pltpu.roll(tile, 64, 1)

    def corners(k):
        accs = [jnp.zeros((8, 128), f32), jnp.zeros((8, 128), f32)]
        for t in range(TILES):
            for c in range(3):
                base = 8 * (t % 16) + 2 * c
                both = jnp.where(lane == 127, V[c, 0, rows(t)], V[c, PLANES - 1, rows(t)])
                hit = jnp.logical_or(lane == base, lane == base + 1)
                accs[t // 16] = jnp.where(hit, pltpu.roll(both, base + 1, 1), accs[t // 16])
        for g in range(2):
            CK[k, pl.ds(8 * g, 8)] = accs[g]

    def corner_of(ref, k, t, c, by):
        return pltpu.roll(ref[k, pl.ds(8 * (t // 16), 8)], (by - 8 * (t % 16) - 2 * c) % 128, 1)

    def trial(y, tiles):
        back = (128 - 2 * y) % 128 if isinstance(y, int) else lax.rem(128 - 2 * y, 128)

        def lower_dip(value, i, t):
            halo = SG[i, rows(t)]
            if not isinstance(back, int) or back:
                halo = pltpu.roll(halo, back, 1)
            return value - jnp.where(lane == 0, halo, pltpu.roll(value, 1, 1))

        for t in tiles:
            r = rows(t)
            sxx, szz, sxz, syz, syy, sxy = (S[i, y + 1, r] for i in range(6))
            scale = DT * C[BUO, y + 1, r]
            vx = V[0, y, r] + scale * (
                (sxx - below(S, (XX, y + 1), t)) + (sxy - S[XY, y, r]) + lower_dip(sxz, 1, t)
            )
            vy = V[1, y, r] + scale * (
                (sxy - below(S, (XY, y + 1), t)) + (syy - S[YY, y, r]) + lower_dip(syz, 2, t)
            )
            vz = V[2, y, r] + scale * (
                (sxz - below(S, (XZ, y + 1), t)) + (syz - S[YZ, y, r]) + lower_dip(szz, 0, t)
            )
            V[0, y, r] = vx
            V[1, y, r] = vy
            V[2, y, r] = vz

    def stress(p, here, here_lead, over, over_lead, halo, ghost=False, last=False, tiles=range(TILES)):
        def put(i, value):
            if ghost:
                S[i, p, r] = jnp.where(dn_y, value, S[i, p, r])
            elif last:
                str_out[S_ORDER[i], p - 1, r] = value
            else:
                S[i, p, r] = value

        for t in tiles:
            if last and t == TILES - 1:
                continue
            r = rows(t)

            def upper_dip(value, c):
                return jnp.where(lane == 127, halo(c, t), pltpu.roll(value, 127, 1)) - value

            vx, vy, vz = (here[here_lead(c) + (r,)] for c in range(3))
            ox, oy, oz = (over[over_lead(c) + (r,)] for c in range(3))
            exx = above(here, here_lead(0), t) - vx
            eyy = oy - vy
            ezz = upper_dip(vz, 2)
            c11, c66, c13, c44 = (C[i, p, r] for i in (C11, C66, C13, C44))
            lame = c11 - 2.0 * c66
            put(YY, S[YY, p, r] + DT * (lame * exx + c11 * eyy + c13 * ezz))
            put(YZ, S[YZ, p, r] + DT * c44 * (upper_dip(vy, 1) + (oz - vz)))
            put(XY, S[XY, p, r] + DT * c66 * ((ox - vx) + (above(here, here_lead(1), t) - vy)))
            if not ghost:
                put(XX, S[XX, p, r] + DT * (c11 * exx + lame * eyy + c13 * ezz))
                put(ZZ, S[ZZ, p, r] + DT * (c13 * (exx + eyy) + C[C33, p, r] * ezz))
                put(XZ, S[XZ, p, r] + DT * c44 * (
                    upper_dip(vx, 0) + (above(here, here_lead(2), t) - vz)
                ))

    def next_dip(y):
        return lambda c, t: pltpu.roll(UN[rows(t)], 126 - 16 * c - 2 * y, 1)

    def stress_own(k, tiles, y):
        stress(
            y + 1, V, lambda c: (c, y), V, lambda c: (c, y + 1), next_dip(y),
            last=k == STEPS - 1, tiles=tiles,
        )

    def stress_last(k):
        stress(PLANES, V, lambda c: (c, PLANES - 1), VN, lambda c: (k, c), next_dip(PLANES - 1), last=k == STEPS - 1)

    def stress_ghost(k):
        stress(0, VP, lambda c: (k, c), V, lambda c: (c, 0), lambda c, t: corner_of(ZD2, k, t, c, 126), ghost=True)

    def column_ghost(early):
        in_time = jnp.logical_and(lane >= 2, lane < 12)
        for t in range(1, TILES - 3) if early else range(TILES):
            r = rows(t)

            def put(i, value, corner):
                skip = lane == 14 if corner else None
                if early:
                    skip = jnp.logical_not(in_time)
                elif 1 <= t < TILES - 3:
                    skip = jnp.logical_or(in_time, skip) if corner else in_time
                SG[i, r] = value if skip is None else jnp.where(skip, SG[i, r], value)

            def shifted(ref, by):
                return pltpu.roll(ref[r], by % 128, 1)

            def upper_rows(c):
                if t in (TILES - 2, TILES - 1):
                    return pltpu.roll(
                        jnp.where(sub == 7, 0.0, pltpu.roll(UM[r], 7, 0)), (-16 * c) % 128, 1
                    )
                return pltpu.roll(UM[pl.ds(8 * t + 1, 8)], (-16 * c) % 128, 1)

            vx, vy, vz = UM[r], shifted(UM, -16), shifted(UM, -32)
            ox, oy, oz = shifted(UO, -1), shifted(UO, -17), shifted(UO, -33)
            exx = upper_rows(0) - vx
            eyy = pltpu.roll(vy, 126, 1) - vy
            ezz = oz - vz
            c13, c44, c33 = CG[0, r], CG[1, r], CG[2, r]
            zz = SG[0, r] + DT * (c13 * (exx + eyy) + c33 * ezz)
            yz = SG[2, r] + DT * c44 * ((oy - vy) + (pltpu.roll(vz, 126, 1) - vz))
            xz = SG[1, r] + DT * c44 * ((ox - vx) + (upper_rows(2) - vz))
            put(0, zz, True)
            put(1, xz, False)
            put(2, yz, True)
            if early:
                continue
            for i, value in enumerate((exx, vy, ezz, oy - vy, vz)):
                GP[i, r] = value

    def column_corner(k):
        here = jnp.logical_and(lane == 14, dn_z)
        for t in range(TILES):
            r = rows(t)
            exx, vy, ezz, oy_vy, vz = (GP[i, r] for i in range(5))
            eyy = corner_of(ZD1, k, t, 1, 14) - vy
            c13, c44, c33 = CG[0, r], CG[1, r], CG[2, r]
            zz = SG[0, r] + DT * (c13 * (exx + eyy) + c33 * ezz)
            yz = SG[2, r] + DT * c44 * (oy_vy + (corner_of(ZD1, k, t, 2, 14) - vz))
            SG[0, r] = jnp.where(here, zz, SG[0, r])
            SG[2, r] = jnp.where(here, yz, SG[2, r])

    def fault():
        for c in range(3):
            for y in range(PLANES):
                FB[c, pl.ds(y, 1)] = V[c, y, pl.ds(own_f, 1)]
                FB[3 + c, pl.ds(y, 1)] = V[c, y, pl.ds(other_f, 1)]
        own_v, other_v = [FB[c] for c in range(3)], [FB[3 + c] for c in range(3)]
        own_b, other_b = FB[6], FB[7]
        minus_b = jnp.where(is_minus, own_b, other_b)
        plus_b = jnp.where(is_minus, other_b, own_b)
        minus_v = [jnp.where(is_minus, a, b) for a, b in zip(own_v, other_v)]
        plus_v = [jnp.where(is_minus, b, a) for a, b in zip(own_v, other_v)]
        impedance = 1.0 / (DT * (minus_b + plus_b))
        jump = [b - a for a, b in zip(minus_v, plus_v)]
        locked_y = pre[0] + impedance * jump[1]
        locked_z = pre[1] + impedance * jump[2]
        magnitude = jnp.sqrt(locked_y * locked_y + locked_z * locked_z + 1.0)
        hold = strength[...]
        rate = inv[...]
        value = slip[...]
        for _ in range(NEWTON):
            scaled = rate * value
            size = jnp.abs(scaled)
            root = jnp.sqrt(size * size + 1.0)
            log = jnp.log(size + root)
            residual = magnitude - impedance * value - hold * jnp.where(scaled < 0.0, -log, log)
            tangent = -impedance - hold * rate / root
            value = value - residual / tangent
        value = value * mask[...].astype(f32)
        slip[...] = value
        retained = 1.0 - impedance * value / magnitude
        traction = [impedance * jump[0], retained * locked_y - pre[0], retained * locked_z - pre[1]]
        for c in range(3):
            minus_new = minus_v[c] + DT * minus_b * traction[c]
            plus_new = plus_v[c] - DT * plus_b * traction[c]
            FB[c] = jnp.where(is_minus, minus_new, plus_new)
            FB[3 + c] = jnp.where(is_minus, plus_new, minus_new)
        for c in range(3):
            for y in range(PLANES):
                V[c, y, pl.ds(own_f, 1)] = FB[c, pl.ds(y, 1)]
                V[c, y, pl.ds(other_f, 1)] = FB[3 + c, pl.ds(y, 1)]

    @pl.when(jnp.logical_not(up_y))
    def _():
        VN[...] = jnp.zeros(VN.shape, f32)
        ZD1[...] = jnp.zeros(ZD1.shape, f32)

    @pl.when(jnp.logical_not(dn_y))
    def _():
        S[pl.ds(YZ, 3), 0] = jnp.zeros((3, EXT, 128), f32)

    @pl.when(jnp.logical_not(up_z))
    def _():
        ZN[...] = jnp.zeros(ZN.shape, f32)
        ZD2[...] = jnp.zeros(ZD2.shape, f32)

    @pl.when(jnp.logical_not(dn_z))
    def _():
        SG[...] = jnp.zeros(SG.shape, f32)

    ghost_rows = pl.ds(ROWS, 8)
    strike = pl.ds(YZ, 3)
    strike_c = pl.ds(C11, 4)
    for i in (YZ, YY, XY):
        loads["s7", i].wait()
    for i in range(6):
        loads["se", i].wait()
    loads["ve"].wait()
    for i in range(6):
        loads["ce", i].wait()
    fields = [(SE, S, i, 1) for i in range(6)] + [(VE, V, i, 0) for i in range(3)]
    fields += [(CE, C, i, 1) for i in range(6)]
    for n, (src, _, i, _) in enumerate(fields):
        for q in range(PLANES // 2):
            first, second = src[i, 2 * q], src[i, 2 * q + 1]
            low = jnp.where(is_minus, pltpu.roll(first, 4, 0), first)
            high = jnp.where(is_minus, second, pltpu.roll(second, 4, 0))
            XS[n, q] = jnp.where(sub < 4, low, high)

    def spread(n):
        _, dst, i, base = fields[n]
        for q in range(PLANES // 2):
            value = XR[n, q]
            moved = pltpu.roll(value, 4, 0)
            dst[i, base + 2 * q, ghost_rows] = jnp.where(is_minus, value, moved)
            dst[i, base + 2 * q + 1, ghost_rows] = jnp.where(is_minus, moved, value)

    for i in (ZZ, XZ, YZ, YY, XY, XX):
        loads["s", i].wait()
    accs = pack(S, ZZ, 1, PI.at[0], 16)
    PI[0, pl.ds(64, 8)] = jnp.where(is_minus, pltpu.roll(accs[7], 64, 1), accs[0])
    pl.semaphore_wait(barrier, count)
    message("y0", S.at[strike, PLANES, own], S.at[strike, 0, own], 0, 1, 0)
    message("xy0", SE.at[strike, PLANES - 1], S.at[strike, 0, ghost_rows], 1, 1, 0)
    message("xa", XS.at[pl.ds(0, 10)], XR.at[pl.ds(0, 10)], 1, 0, 0)
    message("z0", PI.at[0, pl.ds(0, 64)], ZI.at[0, pl.ds(0, 64)], 0, 0, 1)
    message("xz0", PI.at[0, pl.ds(64, 8)], ZI.at[0, pl.ds(64, 8)], 1, 0, 1)
    loads["v"].wait()
    for i in range(6):
        loads[i].wait()
    message("xc", XS.at[pl.ds(10, 5)], XR.at[pl.ds(10, 5)], 1, 0, 0)
    message("yc", C.at[strike_c, PLANES, own], C.at[strike_c, 0, own], 0, 1, 0)
    message("xyc", CE.at[strike_c, PLANES - 1], C.at[strike_c, 0, ghost_rows], 1, 1, 0)
    accs = pack(C, C13, 1, PI.at[1], 16)
    message("zc", PI.at[1, pl.ds(0, 64)], ZI.at[1, pl.ds(0, 64)], 0, 0, 1)
    PI[1, pl.ds(64, 8)] = jnp.where(is_minus, pltpu.roll(accs[7], 64, 1), accs[0])
    message("xzc", PI.at[1, pl.ds(64, 8)], ZI.at[1, pl.ds(64, 8)], 1, 0, 1)

    for name in ("pre", "mask", "ids", "inv", "slip", "reg_a", "reg_n"):
        loads[name].wait()
    number = ids[...]
    picked_a = jnp.zeros((8, 128), f32)
    picked_n = jnp.zeros((8, 128), f32)
    for i in range(8):
        picked_a = jnp.where(number == i, reg_a[i], picked_a)
        picked_n = jnp.where(number == i, reg_n[i], picked_n)
    strength[...] = picked_a * picked_n

    def columns(src, dst):
        for t in range(TILES):
            tile = src[pl.ds(8 * (t // 2), 8)]
            for c in range(3):
                shift = (-16 * c - 64 * (t % 2)) % 128
                dst[c, rows(t)] = pltpu.roll(tile, shift, 1) if shift else tile

    arrived("z0")
    arrived("xz0")

    @pl.when(dn_z)
    def _():
        columns(ZI.at[0], SG)

    own_tiles = range(TILES - 1)
    all_tiles = range(TILES)

    def planes(first, last, body):
        def step(y, carry):
            body(y)
            return carry

        lax.fori_loop(first, last, step, 0)

    planes(1, PLANES, lambda y: trial(y, own_tiles))

    def columns_early(k):
        pack(V, 0, 0, PK.at[k, 0], TILES, early)
        message(("zb1", k), PK.at[k, 0], ZN.at[k, 0], 0, 0, -1)
        if k < STEPS - 1:
            message(("zf1", k), PK.at[k, 0], ZM.at[k, 0], 0, 0, 1)

    columns_early(0)
    arrived("xa")
    for n in range(10):
        spread(n)
    arrived("xy0")
    for y in range(PLANES):
        FB[6, pl.ds(y, 1)] = C[BUO, y + 1, pl.ds(own_f, 1)]
        FB[7, pl.ds(y, 1)] = C[BUO, y + 1, pl.ds(other_f, 1)]
    for y in range(PLANES):
        trial(y, [TILES - 1])
    arrived("y0")
    planes(0, 1, lambda y: trial(y, own_tiles))

    pieces = [(8, 40), (0, 8), (40, EXT)]

    def send_strike(k, chosen):
        for i in chosen:
            some = pl.ds(pieces[i][0], pieces[i][1] - pieces[i][0])
            message(("yb", k, i), V.at[:, 0, some], VN.at[k, :, some], 0, -1, 0)
            if k < STEPS - 1:
                message(("yf", k, i), V.at[:, PLANES - 1, some], VP.at[k, :, some], 0, 1, 0)

    for k in range(STEPS):
        last = k == STEPS - 1
        send_strike(k, [0])
        fault()
        if not last:
            corners(k)
            message(("d1", k), CK.at[k], ZD1.at[k], 0, -1, 1)
            message(("d2", k), CK.at[k], ZD2.at[k], 0, 1, -1)
        send_strike(k, [1, 2])
        pack(V, 0, 0, PK.at[k, 1], TILES, lambda y, t: not early(y, t))
        message(("zb", k), PK.at[k, 1], ZN.at[k, 1], 0, 0, -1)
        if not last:
            message(("zf", k), PK.at[k, 1], ZM.at[k, 1], 0, 0, 1)
        if last:
            slip_out[...] = slip[...]

            def copy_plane(y):
                for c in range(3):
                    vel_out[c, y] = V[c, y, own]

            planes(0, PLANES, copy_plane)
        if k == 0:
            arrived("zc")
            arrived("xzc")

            @pl.when(dn_z)
            def _():
                columns(ZI.at[1], CG)

            arrived("xc")
            for n in range(10, 15):
                spread(n)
            gone("y0")
        arrived(("zb1", k))
        unpack(ZN.at[k, 0], UN)
        planes(1, PLANES - 1, functools.partial(stress_own, k, INNER))
        if not last:
            arrived(("zf1", k))

            @pl.when(dn_z)
            def _():
                unpack(ZM.at[k, 0], UM)
                unpack(PK.at[k, 0], UO)
                column_ghost(True)

            planes(2, PLANES - 2, lambda y: trial(y, range(2, TILES - 3)))
        arrived(("zb", k))
        merge(ZN.at[k], UN)
        for y in range(1, PLANES - 1):
            stress_own(k, FAULT, y)
        stress_own(k, all_tiles, 0)
        if last:
            for i in range(3):
                arrived(("yb", k, i))
            stress_last(k)
            break
        arrived(("zf", k))

        @pl.when(dn_z)
        def _():
            merge(ZM.at[k], UM)
            merge(PK.at[k], UO)
            column_ghost(False)

        for y in range(2, PLANES - 2):
            trial(y, [0, 1, TILES - 3, TILES - 2, TILES - 1])
        planes(0, 2, lambda i: trial(1 + (PLANES - 3) * i, all_tiles))
        columns_early(k + 1)
        if k == 0:
            arrived("yc")
            arrived("xyc")
        arrived(("d1", k))
        arrived(("d2", k))
        for i in range(3):
            for name in ("yf", "yb"):
                gone((name, k, i))
                arrived((name, k, i))
        column_corner(k)
        stress_ghost(k)
        stress_last(k)
        trial(0, all_tiles)
        trial(PLANES - 1, all_tiles)

    for name in list(sent):
        gone(name)


def writer(vel_in, str_in, slip_in, vel_out, str_out, slip_out, sem):
    pairs = [(slip_in, slip_out)]
    pairs += [(str_in.at[i], str_out.at[i]) for i in range(6)]
    pairs += [(vel_in.at[i], vel_out.at[i]) for i in range(3)]
    copies = [pltpu.make_async_copy(src, dst, sem.at[i]) for i, (src, dst) in enumerate(pairs)]
    for copy in copies:
        copy.start()
    for copy in copies:
        copy.wait()


def local(
    velocity, stress, buoyancy, stiff_xx, stiff_xz, stiff_zz, shear_vert, shear_horiz,
    prestress, fault_mask, region_ids, inverse_rate, slip_prev, region_a, region_normal,
):
    f32 = jnp.float32
    hbm = pl.BlockSpec(memory_space=pltpu.HBM)
    vmem = pl.BlockSpec(memory_space=pltpu.VMEM)
    tile = pltpu.VMEM((8, 128), f32)
    plane = (EXT, 128)
    packed = (72, 128)
    corner = (16, 128)
    large = [
        pltpu.with_memory_space_constraint(x, pltpu.HBM)
        for x in (
            velocity, stress, buoyancy, stiff_xx, stiff_xz, stiff_zz, shear_vert, shear_horiz,
            prestress, fault_mask, region_ids, inverse_rate, slip_prev, region_a, region_normal,
        )
    ]
    results = pl.pallas_call(
        kernel,
        out_shape=(
            jax.ShapeDtypeStruct(velocity.shape, f32),
            jax.ShapeDtypeStruct(stress.shape, f32),
            jax.ShapeDtypeStruct(slip_prev.shape, f32),
        ),
        in_specs=[hbm] * 15,
        out_specs=(vmem, vmem, vmem),
        scratch_shapes=[
            pltpu.VMEM((6, PLANES + 1) + plane, f32),
            pltpu.VMEM((3, PLANES) + plane, f32),
            pltpu.VMEM((6, PLANES + 1) + plane, f32),
            pltpu.VMEM((STEPS, 3) + plane, f32),
            pltpu.VMEM((STEPS - 1, 3) + plane, f32),
            pltpu.VMEM((STEPS, 2) + packed, f32),
            pltpu.VMEM((STEPS, 2) + packed, f32),
            pltpu.VMEM((STEPS - 1, 2) + packed, f32),
            pltpu.VMEM((5,) + plane, f32),
            pltpu.VMEM((STEPS - 1,) + corner, f32),
            pltpu.VMEM((STEPS - 1,) + corner, f32),
            pltpu.VMEM((STEPS - 1,) + corner, f32),
            pltpu.VMEM((2,) + packed, f32),
            pltpu.VMEM((2,) + packed, f32),
            pltpu.VMEM(plane, f32),
            pltpu.VMEM(plane, f32),
            pltpu.VMEM(plane, f32),
            pltpu.VMEM((3,) + plane, f32),
            pltpu.VMEM((3,) + plane, f32),
            pltpu.VMEM((8, 8, 128), f32),
            pltpu.VMEM((6, PLANES, 8, 128), f32),
            pltpu.VMEM((3, PLANES, 8, 128), f32),
            pltpu.VMEM((6, PLANES, 8, 128), f32),
            pltpu.VMEM((15, PLANES // 2, 8, 128), f32),
            pltpu.VMEM((15, PLANES // 2, 8, 128), f32),
            pltpu.VMEM((2, 8, 128), f32),
            pltpu.VMEM((8, 128), jnp.int32),
            pltpu.VMEM((8, 128), jnp.int32),
            tile,
            tile,
            tile,
            pltpu.SMEM((8,), f32),
            pltpu.SMEM((8,), f32),
            pltpu.SemaphoreType.DMA((40,)),
            pltpu.SemaphoreType.DMA((56,)),
            pltpu.SemaphoreType.DMA((56,)),
        ],
        compiler_params=pltpu.CompilerParams(
            collective_id=0, has_side_effects=True, vmem_limit_bytes=40 * 1024 * 1024
        ),
        name="rupture",
    )(*large)
    return pl.pallas_call(
        writer,
        out_shape=tuple(jax.ShapeDtypeStruct(x.shape, f32) for x in results),
        in_specs=[vmem] * 3,
        out_specs=(hbm, hbm, hbm),
        scratch_shapes=[pltpu.SemaphoreType.DMA((16,))],
        compiler_params=pltpu.CompilerParams(vmem_limit_bytes=1024 * 1024),
        name="writer",
    )(*results)


def solution(mesh):
    cell, fault_tile = P("gy", "gx", "gz"), P("gy", "gz")
    field = P(None, "gy", "gx", "gz")
    in_specs = (field, field) + (cell,) * 6 + (P(None, "gy", "gz"),) + (fault_tile,) * 4 + (P(), P())
    out_specs = (field, field, fault_tile)
    return jax.shard_map(local, mesh=mesh, in_specs=in_specs, out_specs=out_specs, check_vma=False)
```

```python
import functools

import jax
import jax.numpy as jnp
from jax import lax
from jax.experimental import pallas as pl
from jax.experimental.pallas import tpu as pltpu
from jax.sharding import PartitionSpec as P

STEPS = 3
NEWTON = 3
DT = 0.2
MESH = pl.DeviceIdType.MESH

S_ORDER = (0, 2, 4, 3, 1, 5)
XX, ZZ, XZ, YZ, YY, XY = range(6)
BUO, C11, C66, C13, C44, C33 = range(6)

PLANES = 8
ROWS = 128
TILES = 17
EXT = 8 * TILES
GHOST = slice(ROWS, EXT)


def kernel(
    vel_hbm, str_hbm, buo_hbm, c11_hbm, c13_hbm, c33_hbm, c44_hbm, c66_hbm,
    pre_hbm, mask_hbm, ids_hbm, inv_hbm, slip_hbm, reg_a_hbm, reg_n_hbm,
    vel_out, str_out, slip_out,
    S, V, C, VN, VP, PK, ZN, ZM, GP, CK, ZD1, ZD2, PI, ZI, UN, UM, UO, SG, CG,
    FB, SE, VE, CE, XS, XR, pre, mask, ids, inv, slip, strength, reg_a, reg_n,
    lsem, ssem, rsem,
):
    f32 = jnp.float32
    ngy, ngz = lax.axis_size("gy"), lax.axis_size("gz")
    gx, gy, gz = lax.axis_index("gx"), lax.axis_index("gy"), lax.axis_index("gz")
    is_minus = gx == 0
    lane = lax.broadcasted_iota(jnp.int32, (8, 128), 1)
    sub = lax.broadcasted_iota(jnp.int32, (8, 128), 0)
    edge = (1 - gx) * (ROWS - 8)
    own_f = (1 - gx) * (ROWS - 1)
    other_f = ROWS + gx * 7

    up_y, dn_y, up_z, dn_z = gy < ngy - 1, gy > 0, gz < ngz - 1, gz > 0

    def at(dx, dy, dz):
        return (
            gx if dx == 0 else 1 - gx,
            jnp.clip(gy + dy, 0, ngy - 1),
            jnp.clip(gz + dz, 0, ngz - 1),
        )

    def exists(dy, dz):
        ok = gy >= 0
        if dy:
            ok = jnp.logical_and(ok, up_y if dy > 0 else dn_y)
        if dz:
            ok = jnp.logical_and(ok, up_z if dz > 0 else dn_z)
        return ok

    barrier = pltpu.get_barrier_semaphore()
    around = [
        (0, 1, 0), (0, -1, 0), (0, 0, 1), (0, 0, -1), (0, -1, 1), (0, 1, -1),
        (1, 0, 0), (1, 1, 0), (1, -1, 0), (1, 0, 1), (1, 0, -1),
    ]
    count = jnp.int32(0)
    for dx, dy, dz in around:
        ok = exists(dy, dz)
        count = count + ok.astype(jnp.int32)

        @pl.when(ok)
        def _():
            pl.semaphore_signal(barrier, inc=1, device_id=at(dx, dy, dz), device_id_type=MESH)

    loads = {}

    def load(name, src, dst):
        copy = pltpu.make_async_copy(src, dst, lsem.at[len(loads)])
        copy.start()
        loads[name] = copy

    own = pl.ds(0, ROWS)
    edge_rows = pl.ds(pl.multiple_of(edge, 8), 8)
    for i in range(6):
        load(("se", i), str_hbm.at[S_ORDER[i], :, edge_rows], SE.at[i])
    load("ve", vel_hbm.at[:, :, edge_rows], VE)
    coefficients = ((BUO, buo_hbm), (C11, c11_hbm), (C66, c66_hbm), (C13, c13_hbm), (C44, c44_hbm), (C33, c33_hbm))
    for i, ref in coefficients:
        load(("ce", i), ref.at[:, edge_rows], CE.at[i])
    for i in (YZ, YY, XY):
        load(("s7", i), str_hbm.at[S_ORDER[i], PLANES - 1], S.at[i, PLANES, own])
    for i in (ZZ, XZ):
        load(("s", i), str_hbm.at[S_ORDER[i]], S.at[i, pl.ds(1, PLANES), own])
    for i in (YZ, YY, XY):
        load(("s", i), str_hbm.at[S_ORDER[i], pl.ds(0, PLANES - 1)], S.at[i, pl.ds(1, PLANES - 1), own])
    load(("s", XX), str_hbm.at[S_ORDER[XX]], S.at[XX, pl.ds(1, PLANES), own])
    load("v", vel_hbm, V.at[:, :, own])
    for i, ref in coefficients:
        load(i, ref, C.at[i, pl.ds(1, PLANES), own])
    load("pre", pre_hbm, pre)
    load("mask", mask_hbm, mask)
    load("ids", ids_hbm, ids)
    load("inv", inv_hbm, inv)
    load("slip", slip_hbm, slip)
    load("reg_a", reg_a_hbm, reg_a)
    load("reg_n", reg_n_hbm, reg_n)

    sent = {}

    def message(name, src, dst, dx, dy, dz):
        i = len(sent)
        copy = pltpu.make_async_remote_copy(
            src_ref=src, dst_ref=dst, send_sem=ssem.at[i], recv_sem=rsem.at[i],
            device_id=at(dx, dy, dz), device_id_type=MESH,
        )
        sent[name] = [copy, exists(dy, dz), exists(-dy, -dz), True]

        @pl.when(exists(dy, dz))
        def _():
            copy.start()

    def arrived(name):
        copy, _, source, _ = sent[name]

        @pl.when(source)
        def _():
            copy.wait_recv()

    def gone(name):
        copy, target, _, pending = sent[name]
        if pending:
            sent[name][3] = False

            @pl.when(target)
            def _():
                copy.wait_send()

    def rows(t):
        return pl.ds(8 * t, 8)

    def below(ref, lead, t):
        if t in (0, TILES - 1):
            return jnp.where(sub == 0, 0.0, pltpu.roll(ref[lead + (rows(t),)], 1, 0))
        return ref[lead + (pl.ds(8 * t - 1, 8),)]

    def above(ref, lead, t):
        if t in (TILES - 2, TILES - 1):
            return jnp.where(sub == 7, 0.0, pltpu.roll(ref[lead + (rows(t),)], 7, 0))
        return ref[lead + (pl.ds(8 * t + 1, 8),)]

    def pack(ref, lead, plane0, out, tiles, pick=lambda y, t: True):
        groups = (tiles + 1) // 2

        def body(c, accs):
            accs = list(accs)
            for y in range(PLANES):
                for t in range(tiles):
                    if not pick(y, t):
                        continue
                    base = 64 * (t % 2) + 16 * c + 2 * y
                    moved = pltpu.roll(ref[lead + c, plane0 + y, rows(t)], base + 1, 1)
                    hit = jnp.logical_or(lane == base, lane == base + 1)
                    accs[t // 2] = jnp.where(hit, moved, accs[t // 2])
            return tuple(accs)

        accs = lax.fori_loop(0, 3, body, tuple(jnp.zeros((8, 128), f32) for _ in range(groups)))
        for g in range(groups):
            out[pl.ds(8 * g, 8)] = accs[g]
        return accs

    FAULT = (0, TILES - 2, TILES - 1)
    INNER = range(1, TILES - 2)

    def early(y, t):
        return 0 < y < PLANES - 1 and t in INNER

    def merge(src, dst):
        strike_index = lax.rem(lane, 16) // 2
        outer = jnp.logical_or(strike_index == 0, strike_index == PLANES - 1)
        for g in range((TILES + 1) // 2):
            late = outer
            if 2 * g in FAULT:
                late = jnp.logical_or(late, lane < 64)
            if 2 * g + 1 in FAULT:
                late = jnp.logical_or(late, lane >= 64)
            tile = jnp.where(late, src[1, pl.ds(8 * g, 8)], src[0, pl.ds(8 * g, 8)])
            dst[rows(2 * g)] = tile
            if 2 * g + 1 < TILES:
                dst[rows(2 * g + 1)] = pltpu.roll(tile, 64, 1)

    def unpack(src, dst):
        for t in range(TILES):
            tile = src[pl.ds(8 * (t // 2), 8)]
            dst[rows(t)] = tile if t % 2 == 0 else pltpu.roll(tile, 64, 1)

    def corners(k):
        accs = [jnp.zeros((8, 128), f32), jnp.zeros((8, 128), f32)]
        for t in range(TILES):
            for c in range(3):
                base = 8 * (t % 16) + 2 * c
                both = jnp.where(lane == 127, V[c, 0, rows(t)], V[c, PLANES - 1, rows(t)])
                hit = jnp.logical_or(lane == base, lane == base + 1)
                accs[t // 16] = jnp.where(hit, pltpu.roll(both, base + 1, 1), accs[t // 16])
        for g in range(2):
            CK[k, pl.ds(8 * g, 8)] = accs[g]

    def corner_of(ref, k, t, c, by):
        return pltpu.roll(ref[k, pl.ds(8 * (t // 16), 8)], (by - 8 * (t % 16) - 2 * c) % 128, 1)

    def trial(y, tiles):
        back = (128 - 2 * y) % 128 if isinstance(y, int) else lax.rem(128 - 2 * y, 128)

        def lower_dip(value, i, t):
            halo = SG[i, rows(t)]
            if not isinstance(back, int) or back:
                halo = pltpu.roll(halo, back, 1)
            return value - jnp.where(lane == 0, halo, pltpu.roll(value, 1, 1))

        for t in tiles:
            r = rows(t)
            sxx, szz, sxz, syz, syy, sxy = (S[i, y + 1, r] for i in range(6))
            scale = DT * C[BUO, y + 1, r]
            vx = V[0, y, r] + scale * (
                (sxx - below(S, (XX, y + 1), t)) + (sxy - S[XY, y, r]) + lower_dip(sxz, 1, t)
            )
            vy = V[1, y, r] + scale * (
                (sxy - below(S, (XY, y + 1), t)) + (syy - S[YY, y, r]) + lower_dip(syz, 2, t)
            )
            vz = V[2, y, r] + scale * (
                (sxz - below(S, (XZ, y + 1), t)) + (syz - S[YZ, y, r]) + lower_dip(szz, 0, t)
            )
            V[0, y, r] = vx
            V[1, y, r] = vy
            V[2, y, r] = vz

    def stress(p, here, here_lead, over, over_lead, halo, ghost=False, last=False, tiles=range(TILES)):
        def put(i, value):
            if ghost:
                S[i, p, r] = jnp.where(dn_y, value, S[i, p, r])
            elif last:
                str_out[S_ORDER[i], p - 1, r] = value
            else:
                S[i, p, r] = value

        for t in tiles:
            if last and t == TILES - 1:
                continue
            r = rows(t)

            def upper_dip(value, c):
                return jnp.where(lane == 127, halo(c, t), pltpu.roll(value, 127, 1)) - value

            vx, vy, vz = (here[here_lead(c) + (r,)] for c in range(3))
            ox, oy, oz = (over[over_lead(c) + (r,)] for c in range(3))
            exx = above(here, here_lead(0), t) - vx
            eyy = oy - vy
            ezz = upper_dip(vz, 2)
            c11, c66, c13, c44 = (C[i, p, r] for i in (C11, C66, C13, C44))
            lame = c11 - 2.0 * c66
            put(YY, S[YY, p, r] + DT * (lame * exx + c11 * eyy + c13 * ezz))
            put(YZ, S[YZ, p, r] + DT * c44 * (upper_dip(vy, 1) + (oz - vz)))
            put(XY, S[XY, p, r] + DT * c66 * ((ox - vx) + (above(here, here_lead(1), t) - vy)))
            if not ghost:
                put(XX, S[XX, p, r] + DT * (c11 * exx + lame * eyy + c13 * ezz))
                put(ZZ, S[ZZ, p, r] + DT * (c13 * (exx + eyy) + C[C33, p, r] * ezz))
                put(XZ, S[XZ, p, r] + DT * c44 * (
                    upper_dip(vx, 0) + (above(here, here_lead(2), t) - vz)
                ))

    def next_dip(y):
        return lambda c, t: pltpu.roll(UN[rows(t)], 126 - 16 * c - 2 * y, 1)

    def stress_own(k, tiles, y):
        stress(
            y + 1, V, lambda c: (c, y), V, lambda c: (c, y + 1), next_dip(y),
            last=k == STEPS - 1, tiles=tiles,
        )

    def stress_last(k):
        stress(PLANES, V, lambda c: (c, PLANES - 1), VN, lambda c: (k, c), next_dip(PLANES - 1), last=k == STEPS - 1)

    def stress_ghost(k):
        stress(0, VP, lambda c: (k, c), V, lambda c: (c, 0), lambda c, t: corner_of(ZD2, k, t, c, 126), ghost=True)

    def column_ghost():
        for t in range(TILES):
            r = rows(t)

            def shifted(ref, by):
                return pltpu.roll(ref[r], by % 128, 1)

            def upper_rows(c):
                if t in (TILES - 2, TILES - 1):
                    return pltpu.roll(
                        jnp.where(sub == 7, 0.0, pltpu.roll(UM[r], 7, 0)), (-16 * c) % 128, 1
                    )
                return pltpu.roll(UM[pl.ds(8 * t + 1, 8)], (-16 * c) % 128, 1)

            vx, vy, vz = UM[r], shifted(UM, -16), shifted(UM, -32)
            ox, oy, oz = shifted(UO, -1), shifted(UO, -17), shifted(UO, -33)
            exx = upper_rows(0) - vx
            eyy = pltpu.roll(vy, 126, 1) - vy
            ezz = oz - vz
            c13, c44, c33 = CG[0, r], CG[1, r], CG[2, r]
            zz = SG[0, r] + DT * (c13 * (exx + eyy) + c33 * ezz)
            yz = SG[2, r] + DT * c44 * ((oy - vy) + (pltpu.roll(vz, 126, 1) - vz))
            SG[0, r] = jnp.where(lane == 14, SG[0, r], zz)
            SG[1, r] = SG[1, r] + DT * c44 * ((ox - vx) + (upper_rows(2) - vz))
            SG[2, r] = jnp.where(lane == 14, SG[2, r], yz)
            for i, value in enumerate((exx, vy, ezz, oy - vy, vz)):
                GP[i, r] = value

    def column_corner(k):
        here = jnp.logical_and(lane == 14, dn_z)
        for t in range(TILES):
            r = rows(t)
            exx, vy, ezz, oy_vy, vz = (GP[i, r] for i in range(5))
            eyy = corner_of(ZD1, k, t, 1, 14) - vy
            c13, c44, c33 = CG[0, r], CG[1, r], CG[2, r]
            zz = SG[0, r] + DT * (c13 * (exx + eyy) + c33 * ezz)
            yz = SG[2, r] + DT * c44 * (oy_vy + (corner_of(ZD1, k, t, 2, 14) - vz))
            SG[0, r] = jnp.where(here, zz, SG[0, r])
            SG[2, r] = jnp.where(here, yz, SG[2, r])

    def fault():
        for c in range(3):
            for y in range(PLANES):
                FB[c, pl.ds(y, 1)] = V[c, y, pl.ds(own_f, 1)]
                FB[3 + c, pl.ds(y, 1)] = V[c, y, pl.ds(other_f, 1)]
        own_v, other_v = [FB[c] for c in range(3)], [FB[3 + c] for c in range(3)]
        own_b, other_b = FB[6], FB[7]
        minus_b = jnp.where(is_minus, own_b, other_b)
        plus_b = jnp.where(is_minus, other_b, own_b)
        minus_v = [jnp.where(is_minus, a, b) for a, b in zip(own_v, other_v)]
        plus_v = [jnp.where(is_minus, b, a) for a, b in zip(own_v, other_v)]
        impedance = 1.0 / (DT * (minus_b + plus_b))
        jump = [b - a for a, b in zip(minus_v, plus_v)]
        locked_y = pre[0] + impedance * jump[1]
        locked_z = pre[1] + impedance * jump[2]
        magnitude = jnp.sqrt(locked_y * locked_y + locked_z * locked_z + 1.0)
        hold = strength[...]
        rate = inv[...]
        value = slip[...]
        for _ in range(NEWTON):
            scaled = rate * value
            size = jnp.abs(scaled)
            root = jnp.sqrt(size * size + 1.0)
            log = jnp.log(size + root)
            residual = magnitude - impedance * value - hold * jnp.where(scaled < 0.0, -log, log)
            tangent = -impedance - hold * rate / root
            value = value - residual / tangent
        value = value * mask[...].astype(f32)
        slip[...] = value
        retained = 1.0 - impedance * value / magnitude
        traction = [impedance * jump[0], retained * locked_y - pre[0], retained * locked_z - pre[1]]
        for c in range(3):
            minus_new = minus_v[c] + DT * minus_b * traction[c]
            plus_new = plus_v[c] - DT * plus_b * traction[c]
            FB[c] = jnp.where(is_minus, minus_new, plus_new)
            FB[3 + c] = jnp.where(is_minus, plus_new, minus_new)
        for c in range(3):
            for y in range(PLANES):
                V[c, y, pl.ds(own_f, 1)] = FB[c, pl.ds(y, 1)]
                V[c, y, pl.ds(other_f, 1)] = FB[3 + c, pl.ds(y, 1)]

    @pl.when(jnp.logical_not(up_y))
    def _():
        VN[...] = jnp.zeros(VN.shape, f32)
        ZD1[...] = jnp.zeros(ZD1.shape, f32)

    @pl.when(jnp.logical_not(dn_y))
    def _():
        S[pl.ds(YZ, 3), 0] = jnp.zeros((3, EXT, 128), f32)

    @pl.when(jnp.logical_not(up_z))
    def _():
        ZN[...] = jnp.zeros(ZN.shape, f32)
        ZD2[...] = jnp.zeros(ZD2.shape, f32)

    @pl.when(jnp.logical_not(dn_z))
    def _():
        SG[...] = jnp.zeros(SG.shape, f32)

    ghost_rows = pl.ds(ROWS, 8)
    strike = pl.ds(YZ, 3)
    strike_c = pl.ds(C11, 4)
    for i in (YZ, YY, XY):
        loads["s7", i].wait()
    for i in range(6):
        loads["se", i].wait()
    loads["ve"].wait()
    for i in range(6):
        loads["ce", i].wait()
    fields = [(SE, S, i, 1) for i in range(6)] + [(VE, V, i, 0) for i in range(3)]
    fields += [(CE, C, i, 1) for i in range(6)]
    for n, (src, _, i, _) in enumerate(fields):
        for q in range(PLANES // 2):
            first, second = src[i, 2 * q], src[i, 2 * q + 1]
            low = jnp.where(is_minus, pltpu.roll(first, 4, 0), first)
            high = jnp.where(is_minus, second, pltpu.roll(second, 4, 0))
            XS[n, q] = jnp.where(sub < 4, low, high)

    def spread(n):
        _, dst, i, base = fields[n]
        for q in range(PLANES // 2):
            value = XR[n, q]
            moved = pltpu.roll(value, 4, 0)
            dst[i, base + 2 * q, ghost_rows] = jnp.where(is_minus, value, moved)
            dst[i, base + 2 * q + 1, ghost_rows] = jnp.where(is_minus, moved, value)

    for i in (ZZ, XZ, YZ, YY, XY, XX):
        loads["s", i].wait()
    accs = pack(S, ZZ, 1, PI.at[0], 16)
    PI[0, pl.ds(64, 8)] = jnp.where(is_minus, pltpu.roll(accs[7], 64, 1), accs[0])
    pl.semaphore_wait(barrier, count)
    message("y0", S.at[strike, PLANES, own], S.at[strike, 0, own], 0, 1, 0)
    message("xy0", SE.at[strike, PLANES - 1], S.at[strike, 0, ghost_rows], 1, 1, 0)
    message("xa", XS.at[pl.ds(0, 10)], XR.at[pl.ds(0, 10)], 1, 0, 0)
    message("z0", PI.at[0, pl.ds(0, 64)], ZI.at[0, pl.ds(0, 64)], 0, 0, 1)
    message("xz0", PI.at[0, pl.ds(64, 8)], ZI.at[0, pl.ds(64, 8)], 1, 0, 1)
    loads["v"].wait()
    for i in range(6):
        loads[i].wait()
    message("xc", XS.at[pl.ds(10, 5)], XR.at[pl.ds(10, 5)], 1, 0, 0)
    message("yc", C.at[strike_c, PLANES, own], C.at[strike_c, 0, own], 0, 1, 0)
    message("xyc", CE.at[strike_c, PLANES - 1], C.at[strike_c, 0, ghost_rows], 1, 1, 0)
    accs = pack(C, C13, 1, PI.at[1], 16)
    message("zc", PI.at[1, pl.ds(0, 64)], ZI.at[1, pl.ds(0, 64)], 0, 0, 1)
    PI[1, pl.ds(64, 8)] = jnp.where(is_minus, pltpu.roll(accs[7], 64, 1), accs[0])
    message("xzc", PI.at[1, pl.ds(64, 8)], ZI.at[1, pl.ds(64, 8)], 1, 0, 1)

    for name in ("pre", "mask", "ids", "inv", "slip", "reg_a", "reg_n"):
        loads[name].wait()
    number = ids[...]
    picked_a = jnp.zeros((8, 128), f32)
    picked_n = jnp.zeros((8, 128), f32)
    for i in range(8):
        picked_a = jnp.where(number == i, reg_a[i], picked_a)
        picked_n = jnp.where(number == i, reg_n[i], picked_n)
    strength[...] = picked_a * picked_n

    def columns(src, dst):
        for t in range(TILES):
            tile = src[pl.ds(8 * (t // 2), 8)]
            for c in range(3):
                shift = (-16 * c - 64 * (t % 2)) % 128
                dst[c, rows(t)] = pltpu.roll(tile, shift, 1) if shift else tile

    arrived("z0")
    arrived("xz0")

    @pl.when(dn_z)
    def _():
        columns(ZI.at[0], SG)

    own_tiles = range(TILES - 1)
    all_tiles = range(TILES)

    def planes(first, last, body):
        def step(y, carry):
            body(y)
            return carry

        lax.fori_loop(first, last, step, 0)

    planes(1, PLANES, lambda y: trial(y, own_tiles))

    def pairs(body):
        def both(i):
            body(2 * i + 1)
            body(2 * i + 2)

        planes(0, PLANES // 2 - 1, both)

    def columns_early(k):
        pack(V, 0, 0, PK.at[k, 0], TILES, early)
        message(("zb1", k), PK.at[k, 0], ZN.at[k, 0], 0, 0, -1)
        if k < STEPS - 1:
            message(("zf1", k), PK.at[k, 0], ZM.at[k, 0], 0, 0, 1)

    columns_early(0)
    arrived("xa")
    for n in range(10):
        spread(n)
    arrived("xy0")
    for y in range(PLANES):
        FB[6, pl.ds(y, 1)] = C[BUO, y + 1, pl.ds(own_f, 1)]
        FB[7, pl.ds(y, 1)] = C[BUO, y + 1, pl.ds(other_f, 1)]
    for y in range(PLANES):
        trial(y, [TILES - 1])
    arrived("y0")
    planes(0, 1, lambda y: trial(y, own_tiles))

    pieces = [(8, 40), (0, 8), (40, EXT)]

    def send_strike(k, chosen):
        for i in chosen:
            some = pl.ds(pieces[i][0], pieces[i][1] - pieces[i][0])
            message(("yb", k, i), V.at[:, 0, some], VN.at[k, :, some], 0, -1, 0)
            if k < STEPS - 1:
                message(("yf", k, i), V.at[:, PLANES - 1, some], VP.at[k, :, some], 0, 1, 0)

    for k in range(STEPS):
        last = k == STEPS - 1
        send_strike(k, [0])
        fault()
        if not last:
            corners(k)
            message(("d1", k), CK.at[k], ZD1.at[k], 0, -1, 1)
            message(("d2", k), CK.at[k], ZD2.at[k], 0, 1, -1)
        send_strike(k, [1, 2])
        pack(V, 0, 0, PK.at[k, 1], TILES, lambda y, t: not early(y, t))
        message(("zb", k), PK.at[k, 1], ZN.at[k, 1], 0, 0, -1)
        if not last:
            message(("zf", k), PK.at[k, 1], ZM.at[k, 1], 0, 0, 1)
        if last:
            slip_out[...] = slip[...]

            def copy_plane(y):
                for c in range(3):
                    vel_out[c, y] = V[c, y, own]

            planes(0, PLANES, copy_plane)
        if k == 0:
            arrived("zc")
            arrived("xzc")

            @pl.when(dn_z)
            def _():
                columns(ZI.at[1], CG)

            arrived("xc")
            for n in range(10, 15):
                spread(n)
            gone("y0")
        arrived(("zb1", k))
        unpack(ZN.at[k, 0], UN)
        pairs(functools.partial(stress_own, k, INNER))
        arrived(("zb", k))
        merge(ZN.at[k], UN)
        for y in range(1, PLANES - 1):
            stress_own(k, FAULT, y)
        stress_own(k, all_tiles, 0)
        if last:
            for i in range(3):
                arrived(("yb", k, i))
            stress_last(k)
            break
        arrived(("zf1", k))
        arrived(("zf", k))

        @pl.when(dn_z)
        def _():
            merge(ZM.at[k], UM)
            merge(PK.at[k], UO)
            column_ghost()

        pairs(lambda y: trial(y, all_tiles))
        columns_early(k + 1)
        if k == 0:
            arrived("yc")
            arrived("xyc")
        arrived(("d1", k))
        arrived(("d2", k))
        for i in range(3):
            for name in ("yf", "yb"):
                gone((name, k, i))
                arrived((name, k, i))
        column_corner(k)
        stress_ghost(k)
        stress_last(k)
        trial(0, all_tiles)
        trial(PLANES - 1, all_tiles)

    for name in list(sent):
        gone(name)


def writer(vel_in, str_in, slip_in, vel_out, str_out, slip_out, sem):
    pairs = [(slip_in, slip_out)]
    pairs += [(str_in.at[i], str_out.at[i]) for i in range(6)]
    pairs += [(vel_in.at[i], vel_out.at[i]) for i in range(3)]
    copies = [pltpu.make_async_copy(src, dst, sem.at[i]) for i, (src, dst) in enumerate(pairs)]
    for copy in copies:
        copy.start()
    for copy in copies:
        copy.wait()


def local(
    velocity, stress, buoyancy, stiff_xx, stiff_xz, stiff_zz, shear_vert, shear_horiz,
    prestress, fault_mask, region_ids, inverse_rate, slip_prev, region_a, region_normal,
):
    f32 = jnp.float32
    hbm = pl.BlockSpec(memory_space=pltpu.HBM)
    vmem = pl.BlockSpec(memory_space=pltpu.VMEM)
    tile = pltpu.VMEM((8, 128), f32)
    plane = (EXT, 128)
    packed = (72, 128)
    corner = (16, 128)
    large = [
        pltpu.with_memory_space_constraint(x, pltpu.HBM)
        for x in (
            velocity, stress, buoyancy, stiff_xx, stiff_xz, stiff_zz, shear_vert, shear_horiz,
            prestress, fault_mask, region_ids, inverse_rate, slip_prev, region_a, region_normal,
        )
    ]
    results = pl.pallas_call(
        kernel,
        out_shape=(
            jax.ShapeDtypeStruct(velocity.shape, f32),
            jax.ShapeDtypeStruct(stress.shape, f32),
            jax.ShapeDtypeStruct(slip_prev.shape, f32),
        ),
        in_specs=[hbm] * 15,
        out_specs=(vmem, vmem, vmem),
        scratch_shapes=[
            pltpu.VMEM((6, PLANES + 1) + plane, f32),
            pltpu.VMEM((3, PLANES) + plane, f32),
            pltpu.VMEM((6, PLANES + 1) + plane, f32),
            pltpu.VMEM((STEPS, 3) + plane, f32),
            pltpu.VMEM((STEPS - 1, 3) + plane, f32),
            pltpu.VMEM((STEPS, 2) + packed, f32),
            pltpu.VMEM((STEPS, 2) + packed, f32),
            pltpu.VMEM((STEPS - 1, 2) + packed, f32),
            pltpu.VMEM((5,) + plane, f32),
            pltpu.VMEM((STEPS - 1,) + corner, f32),
            pltpu.VMEM((STEPS - 1,) + corner, f32),
            pltpu.VMEM((STEPS - 1,) + corner, f32),
            pltpu.VMEM((2,) + packed, f32),
            pltpu.VMEM((2,) + packed, f32),
            pltpu.VMEM(plane, f32),
            pltpu.VMEM(plane, f32),
            pltpu.VMEM(plane, f32),
            pltpu.VMEM((3,) + plane, f32),
            pltpu.VMEM((3,) + plane, f32),
            pltpu.VMEM((8, 8, 128), f32),
            pltpu.VMEM((6, PLANES, 8, 128), f32),
            pltpu.VMEM((3, PLANES, 8, 128), f32),
            pltpu.VMEM((6, PLANES, 8, 128), f32),
            pltpu.VMEM((15, PLANES // 2, 8, 128), f32),
            pltpu.VMEM((15, PLANES // 2, 8, 128), f32),
            pltpu.VMEM((2, 8, 128), f32),
            pltpu.VMEM((8, 128), jnp.int32),
            pltpu.VMEM((8, 128), jnp.int32),
            tile,
            tile,
            tile,
            pltpu.SMEM((8,), f32),
            pltpu.SMEM((8,), f32),
            pltpu.SemaphoreType.DMA((40,)),
            pltpu.SemaphoreType.DMA((56,)),
            pltpu.SemaphoreType.DMA((56,)),
        ],
        compiler_params=pltpu.CompilerParams(
            collective_id=0, has_side_effects=True, vmem_limit_bytes=40 * 1024 * 1024
        ),
        name="rupture",
    )(*large)
    return pl.pallas_call(
        writer,
        out_shape=tuple(jax.ShapeDtypeStruct(x.shape, f32) for x in results),
        in_specs=[vmem] * 3,
        out_specs=(hbm, hbm, hbm),
        scratch_shapes=[pltpu.SemaphoreType.DMA((16,))],
        compiler_params=pltpu.CompilerParams(vmem_limit_bytes=1024 * 1024),
        name="writer",
    )(*results)


def solution(mesh):
    cell, fault_tile = P("gy", "gx", "gz"), P("gy", "gz")
    field = P(None, "gy", "gx", "gz")
    in_specs = (field, field) + (cell,) * 6 + (P(None, "gy", "gz"),) + (fault_tile,) * 4 + (P(), P())
    out_specs = (field, field, fault_tile)
    return jax.shard_map(local, mesh=mesh, in_specs=in_specs, out_specs=out_specs, check_vma=False)
```
